32 devices in a mesh: dp: 2 (over x), kvh: 4 (over z), seq: 4 (over y, core).
Axes of the slice: x: 2, y: 2, z: 4, core: 2. Of those that a mesh axis runs over, the one named last changes fastest.
Arguments:
- x_hidden: bfloat16 [256, 4096], P('dp'), parts along dimension 0
- seq_lens: int32 [256], P('dp'), parts along dimension 0
- k_cache: bfloat16 [256, 1024, 8, 128], P('dp', 'seq', 'kvh'), parts along dimension 0
- v_cache: bfloat16 [256, 1024, 8, 128], P('dp', 'seq', 'kvh'), parts along dimension 0
- w_q: bfloat16 [4096, 32, 128], P(None, ('kvh', 'seq'))
- w_o: bfloat16 [32, 128, 4096], P(('kvh', 'seq'))
Outputs:
- output: bfloat16 [256, 4096], P('dp'), parts along dimension 0
There are 2 independent parts. The reference program is written for one: setup_inputs(seed, part) draws one part's arguments, and reference() takes and returns one part's arrays. A program takes and returns all parts, laid end to end along the dimension named above; an argument that names none is the same for every part.
All inputs are finite; a program needn't handle non-finite values.
Results may differ from the reference program's by a relative error of at most 0.00365571.
Values are sent between devices in bfloat16 or wider.
A program may use at most 1 GiB of HBM per device.

```python
import jax
import jax.numpy as jnp
from jax import lax

BATCH_ROWS = 128
SEQ_LEN = 1024
MODEL_DIM = 4096
QUERY_HEADS = 32
KV_HEADS = 8
HEAD_DIM = 128
ROPE_THETA = 500000
TOKEN_SEGMENTS = 64


def rotate_query(q_raw, seq_lens):
    half_dim = HEAD_DIM // 2
    inv_freq = jnp.power(float(ROPE_THETA), -jnp.arange(half_dim, dtype=jnp.float32) * (2.0 / HEAD_DIM))
    angle = (seq_lens - 1).astype(jnp.float32)[:, None] * inv_freq[None, :]
    cosine = jnp.cos(angle)[:, None, :]
    sine = jnp.sin(angle)[:, None, :]
    first = q_raw[..., :half_dim]
    second = q_raw[..., half_dim:]
    return jnp.concatenate([first * cosine - second * sine, second * cosine + first * sine], axis=-1)


def setup_inputs(seed: int = 0, part: int = 0) -> dict:
    base_key = jax.random.key(seed)
    key_list = jax.random.split(base_key, 4)
    part_list = jax.random.split(jax.random.fold_in(key_list[0], part), 8)
    seg_len = SEQ_LEN // TOKEN_SEGMENTS
    low_len = SEQ_LEN // 4
    x_hidden = jax.random.normal(part_list[0], (BATCH_ROWS, MODEL_DIM), jnp.float32).astype(jnp.bfloat16)
    seq_lens = jax.random.randint(part_list[1], (BATCH_ROWS,), low_len, SEQ_LEN + 1)
    seq_lens = seq_lens.at[0].set(SEQ_LEN).at[1].set(low_len)
    seq_lens = jax.random.permutation(part_list[2], seq_lens)
    noise_shape = (BATCH_ROWS, TOKEN_SEGMENTS, seg_len, KV_HEADS, HEAD_DIM)
    mean_shape = (BATCH_ROWS, TOKEN_SEGMENTS, 1, KV_HEADS, HEAD_DIM)
    key_mean = 1.5 * jax.random.normal(part_list[3], mean_shape, jnp.float32)
    key_noise = jax.random.normal(part_list[4], noise_shape, jnp.float32)
    k_cache = (key_noise + key_mean).reshape(BATCH_ROWS, SEQ_LEN, KV_HEADS, HEAD_DIM).astype(jnp.bfloat16)
    value_mean = jax.random.normal(part_list[5], mean_shape, jnp.float32)
    value_noise = 0.7 * jax.random.normal(part_list[6], noise_shape, jnp.float32)
    v_cache = (value_noise + value_mean).reshape(BATCH_ROWS, SEQ_LEN, KV_HEADS, HEAD_DIM).astype(jnp.bfloat16)
    w_q = (jax.random.normal(key_list[1], (MODEL_DIM, QUERY_HEADS, HEAD_DIM), jnp.float32) * MODEL_DIM ** -0.5).astype(jnp.bfloat16)
    w_o = (jax.random.normal(key_list[2], (QUERY_HEADS, HEAD_DIM, MODEL_DIM), jnp.float32) * (QUERY_HEADS * HEAD_DIM) ** -0.5).astype(jnp.bfloat16)
    return dict(x_hidden=x_hidden, seq_lens=seq_lens, k_cache=k_cache, v_cache=v_cache, w_q=w_q, w_o=w_o)


def reference(x_hidden, seq_lens, k_cache, v_cache, w_q, w_o):
    group_size = QUERY_HEADS // KV_HEADS
    q_raw = jnp.einsum('bd,dhk->bhk', x_hidden.astype(jnp.float32), w_q.astype(jnp.float32))
    q_rot = rotate_query(q_raw, seq_lens).astype(jnp.bfloat16)
    q_flat = q_rot.reshape(BATCH_ROWS * KV_HEADS, group_size, HEAD_DIM)
    k_flat = k_cache.transpose(0, 2, 1, 3).reshape(BATCH_ROWS * KV_HEADS, SEQ_LEN, HEAD_DIM)
    v_flat = v_cache.transpose(0, 2, 1, 3).reshape(BATCH_ROWS * KV_HEADS, SEQ_LEN, HEAD_DIM)
    len_flat = jnp.repeat(seq_lens, KV_HEADS)
    positions = jnp.arange(SEQ_LEN)

    def one_head(operands):
        q_head, k_head, v_head, length = operands
        scores = jnp.dot(q_head, k_head.T, preferred_element_type=jnp.float32) * (HEAD_DIM ** -0.5)
        valid_mask = positions[None, :] < length
        scores = jnp.where(valid_mask, scores, -jnp.inf)
        weights = jnp.exp(scores - jnp.max(scores, axis=-1, keepdims=True))
        weight_sum = jnp.sum(weights, axis=-1, keepdims=True)
        attn = jnp.dot(weights.astype(jnp.bfloat16), v_head, preferred_element_type=jnp.float32) / weight_sum
        return attn.astype(jnp.bfloat16)

    attn = lax.map(one_head, (q_flat, k_flat, v_flat, len_flat)).reshape(BATCH_ROWS, QUERY_HEADS, HEAD_DIM)
    y_sum = jnp.einsum('bhk,hkd->bd', attn.astype(jnp.float32), w_o.astype(jnp.float32))
    return (x_hidden.astype(jnp.float32) + y_sum).astype(jnp.bfloat16)
```

```python
import math

import jax
import jax.numpy as jnp
from jax import lax
from jax.experimental import pallas as pl
from jax.experimental.pallas import tpu as pltpu
from jax.sharding import PartitionSpec as P

ROPE_THETA = 500000.0
NEG = -1e30
FLOOR = -1e29
F32 = jnp.float32
BF16 = jnp.bfloat16
MESH = pl.DeviceIdType.MESH

ROWS = 128
RB = 16
NC = ROWS // RB
T = 256
D = 4096
HD = 128
NW = 8
WR = 2 * D // NW
QH = 2
OR_ = 2 * RB + 8

SK_B, SK_C, SK_D, SK_E, SK_F, SK_G, SK_H = 2, 3, 5, 8, 11, 13, 14


def kernel(lens_s, x_h, k_h, v_h, wq_h, wo_h, out_h,
           x_v, k_v, v_v, wq_v, wf_v, wo_v, len_v, q_all,
           o_send, o_recv, at_own, at_peer, y_keep, y_send, y_recv,
           z_buf, z_recv, out_v,
           s_x, s_wq, s_k, s_v, s_wo, s_out,
           wo_ss, wo_rs, q_ss, q_rs, o_ss, o_rs, a_ss, a_rs, y_ss, y_rs,
           z_ss, z_rs, ez_ss, ez_rs, ey_ss, ey_rs, ec_ss, ec_rs, ed_ss, ed_rs):
    dp = lax.axis_index("dp")
    z = lax.axis_index("kvh")
    s = lax.axis_index("seq")
    yy = s // 2
    cc = s % 2
    half_c = cc * 2048
    own_col = half_c + yy * 1024
    oth_col = half_c + (1 - yy) * 1024
    peer_half = (1 - cc) * 2048

    def seq_dev(d):
        return (dp, z, (s + d) % 4)

    def z_dev(d):
        return (dp, (z + d) % 4, s)

    core_dev = (dp, z, yy * 2 + (1 - cc))
    y_dev = (dp, z, (1 - yy) * 2 + cc)

    barrier = pltpu.get_barrier_semaphore()
    for d in (1, 2, 3):
        pl.semaphore_signal(barrier, inc=1, device_id=seq_dev(d), device_id_type=MESH)
        pl.semaphore_signal(barrier, inc=1, device_id=z_dev(d), device_id_type=MESH)

    x_cp = pltpu.make_async_copy(x_h, x_v, s_x)
    x_cp.start()

    def wq_cp(i):
        return pltpu.make_async_copy(wq_h.at[pl.ds(i * WR, WR)], wq_v.at[pl.ds(i * WR, WR)], s_wq.at[i])

    for i in range(NW):
        wq_cp(i).start()

    def k_cp(c):
        return pltpu.make_async_copy(k_h.at[pl.ds(c * RB, RB)], k_v.at[pl.ds(c * RB, RB)], s_k.at[c])

    def v_cp(c):
        return pltpu.make_async_copy(v_h.at[pl.ds(c * RB, RB)], v_v.at[pl.ds(c * RB, RB)], s_v.at[c])

    def wo_cp(i):
        col = pl.multiple_of(oth_col if i == 0 else own_col, 128)
        return pltpu.make_async_copy(wo_h.at[:, pl.ds(col, 1024)], wo_v.at[i, pl.ds(0, 256)], s_wo.at[i])

    def wo_rcp(i):
        col = pl.multiple_of(peer_half + ((1 - yy) if i == 0 else yy) * 1024, 128)
        return pltpu.make_async_remote_copy(
            wo_h.at[:, pl.ds(col, 1024)], wo_v.at[i, pl.ds(256, 256)],
            wo_ss.at[i], wo_rs.at[i], device_id=core_dev, device_id_type=MESH)

    for c in range(NC):
        k_cp(c).start()
        v_cp(c).start()
        if c == 2:
            for i in range(2):
                wo_cp(i).start()

    sub8 = lax.broadcasted_iota(jnp.int32, (8, 128), 0)
    lane8 = lax.broadcasted_iota(jnp.int32, (8, 128), 1)

    def len_body(g, carry):
        r0 = pl.multiple_of(g * 8, 8)
        acc = jnp.zeros((8, 128), jnp.int32)
        for b in range(8):
            acc = jnp.where(sub8 == b, lens_s[r0 + b], acc)
        len_v[pl.ds(r0, 8), :] = acc
        return carry

    lax.fori_loop(0, ROWS // 8, len_body, 0)

    lane = lax.broadcasted_iota(jnp.int32, (ROWS, HD), 1)
    inv_freq = jnp.exp((lane % 64).astype(F32) * (-math.log(ROPE_THETA) / 64.0))
    angle = (len_v[...] - 1).astype(F32) * inv_freq
    cosv = jnp.cos(angle)
    sinv = jnp.where(lane < 64, -jnp.sin(angle), jnp.sin(angle))

    x_cp.wait()
    q_raw = jnp.zeros((ROWS, 2 * HD), F32)
    for i in range(NW):
        wq_cp(i).wait()
        slot = i % 2
        wf_v[slot] = wq_v[pl.ds(i * WR, WR), :].astype(F32)
        w0 = wf_v[slot, pl.ds(0, WR // 2, 2), :].astype(BF16)
        w1 = wf_v[slot, pl.ds(1, WR // 2, 2), :].astype(BF16)
        w = jnp.concatenate([w0, w1], axis=1)
        q_raw = q_raw + jnp.dot(x_v[:, pl.ds(i * (WR // 2), WR // 2)], w, preferred_element_type=F32)
    for hh in range(2):
        qh = q_raw[:, hh * HD:(hh + 1) * HD]
        rot = pltpu.roll(qh, 64, 1)
        q_all[s, :, hh * HD:(hh + 1) * HD] = (qh * cosv + rot * sinv).astype(BF16)

    pl.semaphore_wait(barrier, 6)

    QR = ROWS // QH

    def q_cp(h, d, src):
        return pltpu.make_async_remote_copy(
            q_all.at[src, pl.ds(h * QR, QR)], q_all.at[src, pl.ds(h * QR, QR)],
            q_ss.at[h, d - 1], q_rs.at[h, d - 1], device_id=seq_dev(d), device_id_type=MESH)

    for h in range(QH):
        for d in (2, 1, 3):
            q_cp(h, d, s).start()
    for i in range(2):
        wo_rcp(i).start()

    scale = HD ** -0.5 * math.log2(math.e)
    col8 = lax.broadcasted_iota(jnp.int32, (8, 2 * T), 1)
    big = 1 << 20
    colkey = [jnp.where(col8 % 2 == n, col8 // 2, big) for n in range(2)]
    t_off = s * T
    row64 = lax.broadcasted_iota(jnp.int32, (64, HD), 0) % 8

    def o_cp(c, d):
        return pltpu.make_async_remote_copy(
            o_send.at[c, (s + d) % 4], o_recv.at[c, d - 1],
            o_ss.at[c, d - 1], o_rs.at[c, d - 1], device_id=seq_dev(d), device_id_type=MESH)

    def stage_a(c):
        for h in range(QH):
            @pl.when(c == h * (NC // QH))
            def _():
                for d in (1, 2, 3):
                    q_cp(h, d, (s + 4 - d) % 4).wait_recv()
        k_cp(c).wait()
        v_cp(c).wait()
        r0 = pl.multiple_of(c * RB, RB)
        qf = [q_all[i, pl.ds(r0, RB), :].astype(F32) for i in range(4)]
        scores = []
        for o in range(2):
            q64 = jnp.concatenate(
                [qf[i][8 * o:8 * o + 8, hh * HD:(hh + 1) * HD] for i in range(4) for hh in range(2)], axis=0)
            lhs = jnp.concatenate([jnp.where(row64 == b, q64, 0.0).astype(BF16) for b in range(8)], axis=1)
            kc = jnp.concatenate([k_v[r0 + 8 * o + b] for b in range(8)], axis=1)
            scores.append(lax.dot_general(lhs, kc, (((1,), (1,)), ((), ())), preferred_element_type=F32))
        probs = []
        ml = [jnp.zeros((8, 128), F32) for _ in range(4)]
        for o in range(2):
            lim = len_v[pl.ds(r0 + 8 * o, 8), :] - t_off
            lim = jnp.concatenate([lim] * 4, axis=1)
            mask = [colkey[n] < lim for n in range(2)]
            ps = []
            for g in range(8):
                zz = jnp.where(mask[g // 4], scores[o][8 * g:8 * g + 8, :] * scale, NEG)
                m = jnp.maximum(jnp.max(zz, axis=1, keepdims=True), FLOOR)
                p = jnp.exp2(zz - m)
                l = jnp.sum(p, axis=1, keepdims=True)
                ml[g // 2] = jnp.where(lane8 == 4 * o + g % 2, m, ml[g // 2])
                ml[g // 2] = jnp.where(lane8 == 4 * o + 2 + g % 2, l, ml[g // 2])
                ps.append(p)
            probs.append(jnp.concatenate(ps, axis=0).astype(BF16))
        for o in range(2):
            vc = jnp.concatenate([v_v[r0 + 8 * o + b] for b in range(8)], axis=1)
            res = jnp.dot(probs[o], vc, preferred_element_type=F32)
            acc = jnp.where(row64 == 0, res[:, :HD], 0.0)
            for b in range(1, 8):
                acc = jnp.where(row64 == b, res[:, b * HD:(b + 1) * HD], acc)
            for i in range(4):
                for hh in range(2):
                    g = 2 * i + hh
                    o_send[c, i, pl.ds(hh * RB + 8 * o, 8), :] = acc[8 * g:8 * g + 8]
        for i in range(4):
            o_send[c, i, pl.ds(2 * RB, 8), :] = ml[i]
        for d in (2, 3, 1):
            o_cp(c, d).start()

    def a_cp(c):
        rows = pl.ds(pl.multiple_of(c * RB, RB), RB)
        return pltpu.make_async_remote_copy(
            at_own.at[rows], at_peer.at[rows], a_ss.at[c], a_rs.at[c],
            device_id=core_dev, device_id_type=MESH)

    def stage_b(c):
        for d in (1, 2, 3):
            o_cp(c, d).wait_recv()
        mls = [o_send[c, s, pl.ds(2 * RB, 8), :]] + [o_recv[c, d, pl.ds(2 * RB, 8), :] for d in range(3)]
        mx = jnp.maximum(jnp.maximum(mls[0], mls[1]), jnp.maximum(mls[2], mls[3]))
        is_m = (lane8 % 4) < 2
        fs = [jnp.exp2(jnp.where(is_m, v - mx, 0.0)) for v in mls]
        tot = sum(f * pltpu.roll(v, 126, 1) for f, v in zip(fs, mls))
        tot = jnp.where(is_m, tot, 1.0)
        gs = [f / tot for f in fs]
        r0 = pl.multiple_of(c * RB, RB)
        for hh in range(2):
            parts = []
            for o in range(2):
                idx = 4 * o + hh
                rows = pl.ds(hh * RB + 8 * o, 8)
                acc = jnp.broadcast_to(gs[0][:, idx:idx + 1], (8, HD)) * o_send[c, s, rows, :]
                for d in range(3):
                    acc = acc + jnp.broadcast_to(gs[d + 1][:, idx:idx + 1], (8, HD)) * o_recv[c, d, rows, :]
                parts.append(acc)
            at_own[pl.ds(r0, RB), hh * HD:(hh + 1) * HD] = jnp.concatenate(parts, axis=0).astype(BF16)
        a_cp(c).start()

    def y_cp(c):
        return pltpu.make_async_remote_copy(
            y_send.at[c], y_recv.at[c], y_ss.at[c], y_rs.at[c], device_id=y_dev, device_id_type=MESH)

    def stage_c(c):
        @pl.when(c == 0)
        def _():
            for i in range(2):
                wo_cp(i).wait()
                wo_rcp(i).wait_recv()
        a_cp(c).wait_recv()
        r0 = pl.multiple_of(c * RB, RB)
        at = jnp.concatenate([at_own[pl.ds(r0, RB), :], at_peer[pl.ds(r0, RB), :]], axis=1)
        y_send[c] = jnp.dot(at, wo_v[0], preferred_element_type=F32)
        y_cp(c).start()
        y_keep[c] = jnp.dot(at, wo_v[1], preferred_element_type=F32)

    def z_cp(c, d):
        return pltpu.make_async_remote_copy(
            z_buf.at[c, (z + d) % 4], z_recv.at[c, d - 1],
            z_ss.at[c, d - 1], z_rs.at[c, d - 1], device_id=z_dev(d), device_id_type=MESH)

    def stage_d(c):
        y_cp(c).wait_recv()
        tot = y_keep[c] + y_recv[c]
        for i in range(4):
            z_buf[c, i] = tot[:, i * 256:(i + 1) * 256]
        for d in (2, 1, 3):
            z_cp(c, d).start()

    def ez_cp(c, d, src):
        rows = pl.ds(pl.multiple_of(c * RB, RB), RB)
        cols = pl.ds(pl.multiple_of(own_col + src * 256, 128), 256)
        return pltpu.make_async_remote_copy(
            out_v.at[rows, cols], out_v.at[rows, cols],
            ez_ss.at[c, d - 1], ez_rs.at[c, d - 1], device_id=z_dev(d), device_id_type=MESH)

    def stage_e(c):
        for d in (1, 2, 3):
            z_cp(c, d).wait_recv()
        r0 = pl.multiple_of(c * RB, RB)
        cols = pl.ds(pl.multiple_of(own_col + z * 256, 128), 256)
        tot = (z_buf[c, z] + z_recv[c, 0]) + (z_recv[c, 1] + z_recv[c, 2])
        out_v[pl.ds(r0, RB), cols] = (x_v[pl.ds(r0, RB), cols].astype(F32) + tot).astype(BF16)
        for d in (2, 1, 3):
            ez_cp(c, d, z).start()

    def quarter(c, col):
        return out_v.at[pl.ds(pl.multiple_of(c * RB, RB), RB), pl.ds(pl.multiple_of(col, 128), 1024)]

    def ey_cp(c, col):
        q = quarter(c, col)
        return pltpu.make_async_remote_copy(q, q, ey_ss.at[c], ey_rs.at[c], device_id=y_dev, device_id_type=MESH)

    def ec_cp(c, col):
        q = quarter(c, col)
        return pltpu.make_async_remote_copy(q, q, ec_ss.at[c], ec_rs.at[c], device_id=core_dev, device_id_type=MESH)

    def ed_cp(c, col):
        q = quarter(c, col)
        return pltpu.make_async_remote_copy(q, q, ed_ss.at[c], ed_rs.at[c], device_id=core_dev, device_id_type=MESH)

    def stage_f(c):
        for d in (1, 2, 3):
            ez_cp(c, d, (z + 4 - d) % 4).wait_recv()
        ey_cp(c, own_col).start()
        ec_cp(c, own_col).start()

    def stage_g(c):
        ey_cp(c, oth_col).wait_recv()
        ed_cp(c, oth_col).start()

    def out_cp(c):
        rows = pl.ds(pl.multiple_of(c * RB, RB), RB)
        return pltpu.make_async_copy(out_v.at[rows], out_h.at[rows], s_out.at[c])

    def stage_h(c):
        ec_cp(c, peer_half + yy * 1024).wait_recv()
        ed_cp(c, peer_half + (1 - yy) * 1024).wait_recv()
        out_cp(c).start()

    stages = ((0, stage_a), (SK_B, stage_b), (SK_C, stage_c), (SK_D, stage_d), (SK_E, stage_e),
              (SK_F, stage_f), (SK_G, stage_g), (SK_H, stage_h))

    def slot_body(k, carry):
        for skew, stage in stages:
            @pl.when(jnp.logical_and(k >= skew, k < NC + skew))
            def _():
                stage(k - skew)
        return carry

    lax.fori_loop(0, NC + SK_H, slot_body, 0)

    for h in range(QH):
        for d in (1, 2, 3):
            q_cp(h, d, s).wait_send()
    for i in range(2):
        wo_rcp(i).wait_send()

    def drain(c, carry):
        for d in (1, 2, 3):
            o_cp(c, d).wait_send()
            z_cp(c, d).wait_send()
            ez_cp(c, d, z).wait_send()
        a_cp(c).wait_send()
        y_cp(c).wait_send()
        ey_cp(c, own_col).wait_send()
        ec_cp(c, own_col).wait_send()
        ed_cp(c, oth_col).wait_send()
        out_cp(c).wait()
        return carry

    lax.fori_loop(0, NC, drain, 0)


def solution(mesh):
    def local_step(x_hidden, seq_lens, k_loc, v_loc, wq_loc, wo_loc):
        k2 = k_loc.reshape(ROWS, 2 * T, HD)
        v2 = v_loc.reshape(ROWS, 2 * T, HD)
        wq2 = wq_loc.reshape(2 * D, HD)
        wo2 = wo_loc.reshape(2 * HD, D)
        dma = pltpu.SemaphoreType.DMA
        any_spec = pl.BlockSpec(memory_space=pl.ANY)
        return pl.pallas_call(
            kernel,
            out_shape=jax.ShapeDtypeStruct((ROWS, D), BF16),
            in_specs=[pl.BlockSpec(memory_space=pltpu.SMEM)] + [any_spec] * 5,
            out_specs=any_spec,
            scratch_shapes=[
                pltpu.VMEM((ROWS, D), BF16),
                pltpu.VMEM((ROWS, 2 * T, HD), BF16),
                pltpu.VMEM((ROWS, 2 * T, HD), BF16),
                pltpu.VMEM((2 * D, HD), BF16),
                pltpu.VMEM((2, WR, HD), F32),
                pltpu.VMEM((2, 512, 1024), BF16),
                pltpu.VMEM((ROWS, 128), jnp.int32),
                pltpu.VMEM((4, ROWS, 2 * HD), BF16),
                pltpu.VMEM((NC, 4, OR_, HD), F32),
                pltpu.VMEM((NC, 3, OR_, HD), F32),
                pltpu.VMEM((ROWS, 2 * HD), BF16),
                pltpu.VMEM((ROWS, 2 * HD), BF16),
                pltpu.VMEM((NC, RB, 1024), F32),
                pltpu.VMEM((NC, RB, 1024), F32),
                pltpu.VMEM((NC, RB, 1024), F32),
                pltpu.VMEM((NC, 4, RB, 256), F32),
                pltpu.VMEM((NC, 3, RB, 256), F32),
                pltpu.VMEM((ROWS, D), BF16),
                dma(()), dma((NW,)), dma((NC,)), dma((NC,)), dma((2,)), dma((NC,)),
                dma((2,)), dma((2,)),
                dma((QH, 3)), dma((QH, 3)),
                dma((NC, 3)), dma((NC, 3)),
                dma((NC,)), dma((NC,)),
                dma((NC,)), dma((NC,)),
                dma((NC, 3)), dma((NC, 3)),
                dma((NC, 3)), dma((NC, 3)),
                dma((NC,)), dma((NC,)),
                dma((NC,)), dma((NC,)),
                dma((NC,)), dma((NC,)),
            ],
            compiler_params=pltpu.CompilerParams(
                collective_id=0, has_side_effects=True, vmem_limit_bytes=60 * 1024 * 1024),
            name="decode",
        )(seq_lens, x_hidden, k2, v2, wq2, wo2)

    return jax.shard_map(
        local_step,
        mesh=mesh,
        in_specs=(P('dp', None), P('dp'), P('dp', 'seq', 'kvh', None), P('dp', 'seq', 'kvh', None),
                  P(None, ('kvh', 'seq'), None), P(('kvh', 'seq'), None, None)),
        out_specs=P('dp', None),
        check_vma=False)
```

```python
import math

import jax
import jax.numpy as jnp
from jax import lax
from jax.experimental import pallas as pl
from jax.experimental.pallas import tpu as pltpu
from jax.sharding import PartitionSpec as P

ROPE_THETA = 500000.0
NEG = -1e30
FLOOR = -1e29
F32 = jnp.float32
BF16 = jnp.bfloat16
MESH = pl.DeviceIdType.MESH

ROWS = 128
RB = 16
NC = ROWS // RB
T = 256
D = 4096
HD = 128
NW = 4
WR = 2 * D // NW
QH = NC
NX = 3
OR_ = 2 * RB + 8

Z_FIRST = (0, 1, 2)
NF = len(Z_FIRST)

WORK = (0.97, 0.17, 0.42, 0.1, 0.08, 0.03, 0.02, 0.01)
LAT = (2.4, 1.1, 2.4, 3.6, 3.4, 2.4, 1.1)
WIRE = (0.86, 0.1, 1.4, 1.4, 0.7, 0.7, 0.1)
LINK = (0, 1, 0, 2, 2, 0, 1)
Z_PATH = {2: (3.6, 2.8, 2), 3: (2.4, 0.35, 0)}
PRIO = (7, 6, 5, 4, 3, 2, 1, 0)
Q_AT, Q_STEP, KV_AT, KV_STEP = 6.0, 0.35, 3.5, 1.27


def event_order():
    ready = {(0, 0): max(Q_AT, KV_AT + KV_STEP)}
    link_free = [0.0, 0.0, 0.0]
    now, order, last = 0.0, [], len(WORK) - 1
    while ready:
        can = [e for e, t in ready.items() if t <= now]
        if not can:
            now = min(ready.values())
            continue
        stage, c = min(can, key=lambda e: (PRIO[e[0]], e[1]))
        del ready[stage, c]
        order.append((stage, c))
        now += WORK[stage] * (0.55 if stage == 0 and c in (0, NC) else 1.0)
        if stage == 0:
            if c < NC:
                n = min(c + 1, NC - 1)
                ready[0, c + 1] = max(Q_AT + Q_STEP * n, KV_AT + KV_STEP * (n + 1))
            if c == 0:
                continue
            c -= 1
        if stage < last:
            lat, wire, link = LAT[stage], WIRE[stage], LINK[stage]
            if c in Z_FIRST and stage in Z_PATH:
                lat, wire, link = Z_PATH[stage]
            start = max(now, link_free[link])
            link_free[link] = start + wire
            ready[stage + 1, c] = start + wire + lat
    return order


def kernel(lens_h, x_h, k_h, v_h, wq_h, wo_h, out_v,
           lens_s, x_v, k_v, v_v, wq_v, wf_v, wo_v, len_v, q_all,
           o_send, o_recv, at_own, at_peer, y_keep, y_send, y_recv,
           z_buf, z_recv, f_buf, f_recv, g_buf, g_recv, s_scr, p_scr,
           s_len, s_x, s_wq, s_k, s_v, s_wo,
           wo_ss, wo_rs, q_ss, q_rs, o_ss, o_rs, a_ss, a_rs, y_ss, y_rs,
           z_ss, z_rs, f_ss, g_ss, ez_ss, ez_rs, ey_ss, ey_rs, ec_ss, ec_rs, ed_ss, ed_rs):
    dp = lax.axis_index("dp")
    z = lax.axis_index("kvh")
    s = lax.axis_index("seq")
    yy = s // 2
    cc = s % 2
    half_c = cc * 2048
    own_col = half_c + yy * 1024
    oth_col = half_c + (1 - yy) * 1024
    peer_half = (1 - cc) * 2048

    def seq_dev(d):
        return (dp, z, (s + d) % 4)

    def z_dev(d):
        return (dp, (z + d) % 4, s)

    def arrived(ref, sem):
        pltpu.make_async_remote_copy(ref, ref, sem, sem, device_id=seq_dev(1), device_id_type=MESH).wait_recv()

    def sent(ref, sem):
        pltpu.make_async_remote_copy(ref, ref, sem, sem, device_id=seq_dev(1), device_id_type=MESH).wait_send()

    core_dev = (dp, z, yy * 2 + (1 - cc))
    y_dev = (dp, z, (1 - yy) * 2 + cc)

    def x_cp(i):
        cols = pl.ds(i * (WR // 2), WR // 2)
        return pltpu.make_async_copy(x_h.at[:, cols], x_v.at[:, cols], s_x.at[i])

    lens_cp = pltpu.make_async_copy(lens_h, lens_s, s_len)
    lens_cp.start()

    def wq_cp(i):
        return pltpu.make_async_copy(wq_h.at[pl.ds(i * WR, WR)], wq_v.at[pl.ds(i * WR, WR)], s_wq.at[i])

    def load_q(i, carry):
        cols = pl.ds(pl.multiple_of(i * (WR // 2), WR // 2), WR // 2)
        rows = pl.ds(pl.multiple_of(i * WR, WR), WR)
        pltpu.make_async_copy(x_h.at[:, cols], x_v.at[:, cols], s_x.at[i]).start()
        pltpu.make_async_copy(wq_h.at[rows], wq_v.at[rows], s_wq.at[i]).start()
        return carry

    lax.fori_loop(0, NW, load_q, 0)

    def k_cp(c):
        return pltpu.make_async_copy(k_h.at[pl.ds(c * RB, RB)], k_v.at[pl.ds(c * RB, RB)], s_k.at[c])

    def v_cp(c):
        return pltpu.make_async_copy(v_h.at[pl.ds(c * RB, RB)], v_v.at[pl.ds(c * RB, RB)], s_v.at[c])

    def wo_cp(i):
        col = pl.multiple_of(oth_col if i == 0 else own_col, 128)
        return pltpu.make_async_copy(wo_h.at[:, pl.ds(col, 1024)], wo_v.at[i, pl.ds(0, 256)], s_wo.at[i])

    def wo_rcp(i):
        col = pl.multiple_of(peer_half + ((1 - yy) if i == 0 else yy) * 1024, 128)
        return pltpu.make_async_remote_copy(
            wo_h.at[:, pl.ds(col, 1024)], wo_v.at[i, pl.ds(256, 256)],
            wo_ss, wo_rs, device_id=core_dev, device_id_type=MESH)

    barrier = pltpu.get_barrier_semaphore()
    for d in (1, 2, 3):
        pl.semaphore_signal(barrier, inc=1, device_id=seq_dev(d), device_id_type=MESH)
        pl.semaphore_signal(barrier, inc=1, device_id=z_dev(d), device_id_type=MESH)

    def load_body(c, carry):
        k_cp(c).start()
        v_cp(c).start()

        @pl.when(c == 2)
        def _():
            for i in range(2):
                wo_cp(i).start()
        return carry

    lax.fori_loop(0, NC, load_body, 0)
    lens_cp.wait()

    sub8 = lax.broadcasted_iota(jnp.int32, (8, 128), 0)
    lane8 = lax.broadcasted_iota(jnp.int32, (8, 128), 1)

    def len_body(g, carry):
        r0 = pl.multiple_of(g * 8, 8)
        acc = jnp.zeros((8, 128), jnp.int32)
        for b in range(8):
            acc = jnp.where(sub8 == b, lens_s[r0 + b], acc)
        len_v[pl.ds(r0, 8), :] = acc
        return carry

    lax.fori_loop(0, ROWS // 8, len_body, 0)

    lane = lax.broadcasted_iota(jnp.int32, (ROWS, HD), 1)
    inv_freq = jnp.exp((lane % 64).astype(F32) * (-math.log(ROPE_THETA) / 64.0))
    angle = (len_v[...] - 1).astype(F32) * inv_freq
    cosv = jnp.cos(angle)
    sinv = jnp.where(lane < 64, -jnp.sin(angle), jnp.sin(angle))

    q_raw = jnp.zeros((ROWS, 2 * HD), F32)
    for i in range(NW):
        x_cp(i).wait()
        wq_cp(i).wait()
        slot = i % 2
        wf_v[slot] = wq_v[pl.ds(i * WR, WR), :].astype(F32)
        w0 = wf_v[slot, pl.ds(0, WR // 2, 2), :].astype(BF16)
        w1 = wf_v[slot, pl.ds(1, WR // 2, 2), :].astype(BF16)
        w = jnp.concatenate([w0, w1], axis=1)
        q_raw = q_raw + jnp.dot(x_v[:, pl.ds(i * (WR // 2), WR // 2)], w, preferred_element_type=F32)
    for hh in range(2):
        qh = q_raw[:, hh * HD:(hh + 1) * HD]
        rot = pltpu.roll(qh, 64, 1)
        q_all[s, :, hh * HD:(hh + 1) * HD] = (qh * cosv + rot * sinv).astype(BF16)

    pl.semaphore_wait(barrier, 6)


    def q_cp(h, d, src):
        return pltpu.make_async_remote_copy(
            q_all.at[src, pl.ds(pl.multiple_of(h * RB, RB), RB)], q_all.at[src, pl.ds(pl.multiple_of(h * RB, RB), RB)],
            q_ss, q_rs.at[h], device_id=seq_dev(d), device_id_type=MESH)

    def send_q(h, carry):
        for d in (2, 1, 3):
            q_cp(h, d, s).start()
        return carry

    lax.fori_loop(0, QH, send_q, 0)
    for i in range(2):
        wo_rcp(i).start()

    scale = HD ** -0.5 * math.log2(math.e)
    col8 = lax.broadcasted_iota(jnp.int32, (8, 2 * T), 1)
    big = 1 << 20
    colkey = [jnp.where(col8 % 2 == n, col8 // 2, big) for n in range(2)]
    t_off = s * T
    row64 = lax.broadcasted_iota(jnp.int32, (64, HD), 0) % 8

    def o_cp(c, d):
        return pltpu.make_async_remote_copy(
            o_send.at[c, (s + d) % 4], o_recv.at[c, d - 1],
            o_ss, o_rs.at[c], device_id=seq_dev(d), device_id_type=MESH)

    def issue_scores(c):
        rows = pl.ds(c * RB, RB)
        arrived(q_all.at[pl.ds(0, 3), rows], q_rs.at[c])
        k_cp(c).wait()
        return pl.multiple_of(c * RB, RB)

    def scores(r0):
        qf = [q_all[i, pl.ds(r0, RB), :].astype(F32) for i in range(4)]
        for o in range(2):
            q64 = jnp.concatenate(
                [qf[i][8 * o:8 * o + 8, hh * HD:(hh + 1) * HD] for i in range(4) for hh in range(2)], axis=0)
            lhs = jnp.concatenate([jnp.where(row64 == b, q64, 0.0).astype(BF16) for b in range(8)], axis=1)
            kn = jnp.concatenate([k_v[r0 + 8 * o + b] for b in range(NX)], axis=1)
            res = lax.dot_general(lhs[:, :NX * HD], kn, (((1,), (1,)), ((), ())), preferred_element_type=F32)
            if NX < 8:
                kt = jnp.concatenate([k_v[r0 + 8 * o + b].T for b in range(NX, 8)], axis=0)
                res = res + jnp.dot(lhs[:, NX * HD:], kt, preferred_element_type=F32)
            s_scr[o] = res

    def softmax(c):
        r0 = pl.multiple_of(c * RB, RB)
        ml = [jnp.zeros((8, 128), F32) for _ in range(4)]
        for o in range(2):
            lim = len_v[pl.ds(r0 + 8 * o, 8), :] - t_off
            lim = jnp.concatenate([lim] * 4, axis=1)
            mask = [colkey[n] < lim for n in range(2)]
            for g2 in range(4):
                ps = []
                for g in (2 * g2, 2 * g2 + 1):
                    zz = jnp.where(mask[g // 4], s_scr[o, 8 * g:8 * g + 8, :] * scale, NEG)
                    m = jnp.maximum(jnp.max(zz, axis=1, keepdims=True), FLOOR)
                    p = jnp.exp2(zz - m)
                    l = jnp.sum(p, axis=1, keepdims=True)
                    ml[g // 2] = jnp.where(lane8 == 4 * o + g % 2, m, ml[g // 2])
                    ml[g // 2] = jnp.where(lane8 == 4 * o + 2 + g % 2, l, ml[g // 2])
                    ps.append(p)
                p_scr[o, 16 * g2:16 * g2 + 16, :] = jnp.concatenate(ps, axis=0).astype(BF16)
        for i in range(4):
            o_send[c, i, pl.ds(2 * RB, 8), :] = ml[i]

    def weighted(c):
        r0 = pl.multiple_of(c * RB, RB)
        for o in range(2):
            vc = jnp.concatenate([v_v[r0 + 8 * o + b] for b in range(8)], axis=1)
            res = jnp.dot(p_scr[o], vc, preferred_element_type=F32)
            acc = jnp.where(row64 == 0, res[:, :HD], 0.0)
            for b in range(1, 8):
                acc = jnp.where(row64 == b, res[:, b * HD:(b + 1) * HD], acc)
            for i in range(4):
                for hh in range(2):
                    g = 2 * i + hh
                    o_send[c, i, pl.ds(hh * RB + 8 * o, 8), :] = acc[8 * g:8 * g + 8]

    def send_o(c):
        for d in (2, 3, 1):
            o_cp(c, d).start()

    def attention(k):
        if k > 0:
            v_cp(k - 1).wait()
        if k < NC:
            r0 = issue_scores(k)
        if k > 0:
            softmax(k - 1)
        if k < NC:
            scores(r0)
        if k > 0:
            weighted(k - 1)
            send_o(k - 1)

    def a_cp(c):
        rows = pl.ds(pl.multiple_of(c * RB, RB), RB)
        return pltpu.make_async_remote_copy(
            at_own.at[rows], at_peer.at[rows], a_ss, a_rs.at[c],
            device_id=core_dev, device_id_type=MESH)

    def stage_b(c):
        arrived(o_recv.at[c], o_rs.at[c])
        mls = [o_send[c, s, pl.ds(2 * RB, 8), :]] + [o_recv[c, d, pl.ds(2 * RB, 8), :] for d in range(3)]
        mx = jnp.maximum(jnp.maximum(mls[0], mls[1]), jnp.maximum(mls[2], mls[3]))
        is_m = (lane8 % 4) < 2
        fs = [jnp.exp2(jnp.where(is_m, v - mx, 0.0)) for v in mls]
        tot = sum(f * pltpu.roll(v, 126, 1) for f, v in zip(fs, mls))
        tot = jnp.where(is_m, tot, 1.0)
        gs = [f / tot for f in fs]
        r0 = pl.multiple_of(c * RB, RB)
        for hh in range(2):
            parts = []
            for o in range(2):
                idx = 4 * o + hh
                rows = pl.ds(hh * RB + 8 * o, 8)
                acc = jnp.broadcast_to(gs[0][:, idx:idx + 1], (8, HD)) * o_send[c, s, rows, :]
                for d in range(3):
                    acc = acc + jnp.broadcast_to(gs[d + 1][:, idx:idx + 1], (8, HD)) * o_recv[c, d, rows, :]
                parts.append(acc)
            at_own[pl.ds(r0, RB), hh * HD:(hh + 1) * HD] = jnp.concatenate(parts, axis=0).astype(BF16)
        a_cp(c).start()

    def y_cp(c):
        return pltpu.make_async_remote_copy(
            y_send.at[c], y_recv.at[c], y_ss, y_rs.at[c], device_id=y_dev, device_id_type=MESH)

    def stage_c(c):
        if c == 0:
            for i in range(2):
                wo_cp(i).wait()
            arrived(wo_v.at[:, pl.ds(256, 256)], wo_rs)
        a_cp(c).wait_recv()
        r0 = pl.multiple_of(c * RB, RB)
        at = jnp.concatenate([at_own[pl.ds(r0, RB), :], at_peer[pl.ds(r0, RB), :]], axis=1)
        if c in Z_FIRST:
            for p in range(2):
                part = jnp.dot(at, wo_v[p], preferred_element_type=F32)
                for i in range(4):
                    f_buf[slot_f(c), i, p] = part[:, i * 256:(i + 1) * 256]
            for d in (2, 1, 3):
                f_cp(c, d).start()
            return
        y_send[c] = jnp.dot(at, wo_v[0], preferred_element_type=F32)
        y_cp(c).start()
        y_keep[c] = jnp.dot(at, wo_v[1], preferred_element_type=F32)

    def slot_f(c):
        return Z_FIRST.index(c)

    def f_cp(c, d):
        i = slot_f(c)
        return pltpu.make_async_remote_copy(
            f_buf.at[i, (z + d) % 4], f_recv.at[i, d - 1],
            f_ss, z_rs.at[c], device_id=z_dev(d), device_id_type=MESH)

    def g_cp(c):
        i = slot_f(c)
        return pltpu.make_async_remote_copy(
            g_buf.at[i, 0], g_recv.at[i], g_ss, y_rs.at[c], device_id=y_dev, device_id_type=MESH)

    def z_cp(c, d):
        return pltpu.make_async_remote_copy(
            z_buf.at[c, (z + d) % 4], z_recv.at[c, d - 1],
            z_ss, z_rs.at[c], device_id=z_dev(d), device_id_type=MESH)

    def stage_d(c):
        if c in Z_FIRST:
            i = slot_f(c)
            arrived(f_recv.at[i], z_rs.at[c])
            g_buf[i] = (f_buf[i, z] + f_recv[i, 0]) + (f_recv[i, 1] + f_recv[i, 2])
            g_cp(c).start()
            return
        y_cp(c).wait_recv()
        tot = y_keep[c] + y_recv[c]
        for i in range(4):
            z_buf[c, i] = tot[:, i * 256:(i + 1) * 256]
        for d in (2, 1, 3):
            z_cp(c, d).start()

    def ez_cp(c, d, src):
        rows = pl.ds(pl.multiple_of(c * RB, RB), RB)
        cols = pl.ds(pl.multiple_of(own_col + src * 256, 128), 256)
        return pltpu.make_async_remote_copy(
            out_v.at[rows, cols], out_v.at[rows, cols],
            ez_ss, ez_rs.at[c], device_id=z_dev(d), device_id_type=MESH)

    def stage_e(c):
        if c in Z_FIRST:
            arrived(g_recv.at[slot_f(c)], y_rs.at[c])
        else:
            arrived(z_recv.at[c], z_rs.at[c])
        r0 = pl.multiple_of(c * RB, RB)
        cols = pl.ds(pl.multiple_of(own_col + z * 256, 128), 256)
        if c in Z_FIRST:
            tot = g_buf[slot_f(c), 1] + g_recv[slot_f(c)]
        else:
            tot = (z_buf[c, z] + z_recv[c, 0]) + (z_recv[c, 1] + z_recv[c, 2])
        out_v[pl.ds(r0, RB), cols] = (x_v[pl.ds(r0, RB), cols].astype(F32) + tot).astype(BF16)
        for d in (2, 1, 3):
            ez_cp(c, d, z).start()

    def quarter(c, col):
        return out_v.at[pl.ds(pl.multiple_of(c * RB, RB), RB), pl.ds(pl.multiple_of(col, 128), 1024)]

    def ey_cp(c, col):
        q = quarter(c, col)
        return pltpu.make_async_remote_copy(q, q, ey_ss, ey_rs.at[c], device_id=y_dev, device_id_type=MESH)

    def ec_cp(c, col):
        q = quarter(c, col)
        return pltpu.make_async_remote_copy(q, q, ec_ss, ec_rs.at[c], device_id=core_dev, device_id_type=MESH)

    def ed_cp(c, col):
        q = quarter(c, col)
        return pltpu.make_async_remote_copy(q, q, ed_ss, ed_rs.at[c], device_id=core_dev, device_id_type=MESH)

    def stage_f(c):
        arrived(out_v.at[pl.ds(c * RB, RB), pl.ds(0, 768)], ez_rs.at[c])
        ey_cp(c, own_col).start()
        ec_cp(c, own_col).start()

    def stage_g(c):
        ey_cp(c, oth_col).wait_recv()
        ed_cp(c, oth_col).start()

    def stage_h(c):
        ec_cp(c, peer_half + yy * 1024).wait_recv()
        ed_cp(c, peer_half + (1 - yy) * 1024).wait_recv()

    stages = (attention, stage_b, stage_c, stage_d, stage_e, stage_f, stage_g, stage_h)
    for stage, c in event_order():
        stages[stage](c)

    sent(q_all.at[pl.ds(0, 3)], q_ss)
    sent(wo_v.at[:, pl.ds(0, 256)], wo_ss)
    sent(o_recv, o_ss)
    sent(at_own, a_ss)
    sent(y_send.at[pl.ds(0, NC - NF)], y_ss)
    sent(z_recv.at[pl.ds(0, NC - NF)], z_ss)
    sent(f_recv, f_ss)
    sent(g_recv, g_ss)
    sent(out_v.at[:, pl.ds(0, 768)], ez_ss)
    for sem in (ey_ss, ec_ss, ed_ss):
        sent(out_v.at[:, pl.ds(0, 1024)], sem)


def solution(mesh):
    def local_step(x_hidden, seq_lens, k_loc, v_loc, wq_loc, wo_loc):
        k2 = k_loc.reshape(ROWS, 2 * T, HD)
        v2 = v_loc.reshape(ROWS, 2 * T, HD)
        wq2 = wq_loc.reshape(2 * D, HD)
        wo2 = wo_loc.reshape(2 * HD, D)
        dma = pltpu.SemaphoreType.DMA
        any_spec = pl.BlockSpec(memory_space=pltpu.HBM)
        return pl.pallas_call(
            kernel,
            out_shape=jax.ShapeDtypeStruct((ROWS, D), BF16),
            in_specs=[any_spec] * 6,
            out_specs=pl.BlockSpec(memory_space=pltpu.VMEM),
            scratch_shapes=[
                pltpu.SMEM((ROWS,), jnp.int32),
                pltpu.VMEM((ROWS, D), BF16),
                pltpu.VMEM((ROWS, 2 * T, HD), BF16),
                pltpu.VMEM((ROWS, 2 * T, HD), BF16),
                pltpu.VMEM((2 * D, HD), BF16),
                pltpu.VMEM((2, WR, HD), F32),
                pltpu.VMEM((2, 512, 1024), BF16),
                pltpu.VMEM((ROWS, 128), jnp.int32),
                pltpu.VMEM((4, ROWS, 2 * HD), BF16),
                pltpu.VMEM((NC, 4, OR_, HD), F32),
                pltpu.VMEM((NC, 3, OR_, HD), F32),
                pltpu.VMEM((ROWS, 2 * HD), BF16),
                pltpu.VMEM((ROWS, 2 * HD), BF16),
                pltpu.VMEM((NC, RB, 1024), F32),
                pltpu.VMEM((NC, RB, 1024), F32),
                pltpu.VMEM((NC, RB, 1024), F32),
                pltpu.VMEM((NC, 4, RB, 256), F32),
                pltpu.VMEM((NC, 3, RB, 256), F32),
                pltpu.VMEM((NF, 4, 2, RB, 256), F32),
                pltpu.VMEM((NF, 3, 2, RB, 256), F32),
                pltpu.VMEM((NF, 2, RB, 256), F32),
                pltpu.VMEM((NF, RB, 256), F32),
                pltpu.VMEM((2, 64, 2 * T), F32),
                pltpu.VMEM((2, 64, 2 * T), BF16),
                dma(()), dma((NW,)), dma((NW,)), dma((NC,)), dma((NC,)), dma((2,)),
                dma(()), dma(()),
                dma(()), dma((NC,)),
                dma(()), dma((NC,)),
                dma(()), dma((NC,)),
                dma(()), dma((NC,)),
                dma(()), dma((NC,)),
                dma(()), dma(()),
                dma(()), dma((NC,)),
                dma(()), dma((NC,)),
                dma(()), dma((NC,)),
                dma(()), dma((NC,)),
            ],
            compiler_params=pltpu.CompilerParams(
                collective_id=0, has_side_effects=True, vmem_limit_bytes=52 * 1024 * 1024),
            name="decode",
        )(seq_lens, x_hidden, k2, v2, wq2, wo2)

    return jax.shard_map(
        local_step,
        mesh=mesh,
        in_specs=(P('dp', None), P('dp'), P('dp', 'seq', 'kvh', None), P('dp', 'seq', 'kvh', None),
                  P(None, ('kvh', 'seq'), None), P(('kvh', 'seq'), None, None)),
        out_specs=P('dp', None),
        check_vma=False)
```

```python
import math

import jax
import jax.numpy as jnp
from jax import lax
from jax.experimental import pallas as pl
from jax.experimental.pallas import tpu as pltpu
from jax.sharding import PartitionSpec as P

ROPE_THETA = 500000.0
NEG = -1e30
FLOOR = -1e29
F32 = jnp.float32
BF16 = jnp.bfloat16
MESH = pl.DeviceIdType.MESH

ROWS = 128
RB = 16
NC = ROWS // RB
T = 256
D = 4096
HD = 128
NW = 4
WR = 2 * D // NW
QH = NC
NX = 3
OR_ = 2 * RB + 8

Z_FIRST = (0, 1, 2)
NF = len(Z_FIRST)

ORDER = (
    (0, 0), (0, 1), (0, 2), (0, 3), (0, 4), (1, 0), (0, 5), (1, 1), (2, 0), (2, 1), (0, 6), (1, 3), (0, 7),
    (2, 3), (1, 4), (1, 2), (0, 8), (2, 2), (2, 4), (1, 5), (3, 0), (1, 6), (2, 5), (2, 6), (3, 3), (3, 1),
    (1, 7), (3, 4), (2, 7), (4, 0), (3, 5), (4, 3), (3, 2), (3, 6), (3, 7), (5, 0), (4, 1), (4, 5), (4, 2),
    (5, 3), (4, 4), (4, 6), (4, 7), (5, 1), (5, 2), (5, 5), (5, 4), (5, 6), (5, 7), (6, 2), (6, 0), (6, 1),
    (6, 5), (6, 4), (7, 1), (6, 6), (7, 0), (6, 7), (6, 3), (7, 2), (7, 4), (7, 6), (7, 7), (7, 5), (7, 3),
)


def kernel(lens_h, x_h, k_h, v_h, wq_h, wo_h, out_v,
           lens_s, x_v, k_v, v_v, wq_v, wf_v, wo_v, len_v, q_all,
           o_send, o_recv, at_own, at_peer, y_keep, y_send, y_recv,
           z_buf, z_recv, f_buf, f_recv, g_buf, g_recv, s_scr, p_scr,
           s_len, s_x, s_wq, s_k, s_v, s_wo,
           wo_ss, wo_rs, q_ss, q_rs, o_ss, o_rs, a_ss, a_rs, y_ss, y_rs,
           z_ss, z_rs, f_ss, g_ss, ez_ss, ez_rs, ey_ss, ey_rs, ec_ss, ec_rs, ed_ss, ed_rs):
    dp = lax.axis_index("dp")
    z = lax.axis_index("kvh")
    s = lax.axis_index("seq")
    yy = s // 2
    cc = s % 2
    half_c = cc * 2048
    own_col = half_c + yy * 1024
    oth_col = half_c + (1 - yy) * 1024
    peer_half = (1 - cc) * 2048

    def seq_dev(d):
        return (dp, z, (s + d) % 4)

    def z_dev(d):
        return (dp, (z + d) % 4, s)

    def arrived(ref, sem):
        pltpu.make_async_remote_copy(ref, ref, sem, sem, device_id=seq_dev(1), device_id_type=MESH).wait_recv()

    def sent(ref, sem):
        pltpu.make_async_remote_copy(ref, ref, sem, sem, device_id=seq_dev(1), device_id_type=MESH).wait_send()

    core_dev = (dp, z, yy * 2 + (1 - cc))
    y_dev = (dp, z, (1 - yy) * 2 + cc)

    def x_cp(i):
        cols = pl.ds(i * (WR // 2), WR // 2)
        return pltpu.make_async_copy(x_h.at[:, cols], x_v.at[:, cols], s_x.at[i])

    lens_cp = pltpu.make_async_copy(lens_h, lens_s, s_len)
    lens_cp.start()

    def wq_cp(i):
        return pltpu.make_async_copy(wq_h.at[pl.ds(i * WR, WR)], wq_v.at[pl.ds(i * WR, WR)], s_wq.at[i])

    def load_q(i, carry):
        cols = pl.ds(pl.multiple_of(i * (WR // 2), WR // 2), WR // 2)
        rows = pl.ds(pl.multiple_of(i * WR, WR), WR)
        pltpu.make_async_copy(x_h.at[:, cols], x_v.at[:, cols], s_x.at[i]).start()
        pltpu.make_async_copy(wq_h.at[rows], wq_v.at[rows], s_wq.at[i]).start()
        return carry

    lax.fori_loop(0, NW, load_q, 0)

    def k_cp(c):
        return pltpu.make_async_copy(k_h.at[pl.ds(c * RB, RB)], k_v.at[pl.ds(c * RB, RB)], s_k.at[c])

    def v_cp(c):
        return pltpu.make_async_copy(v_h.at[pl.ds(c * RB, RB)], v_v.at[pl.ds(c * RB, RB)], s_v.at[c])

    def wo_cp(i):
        col = pl.multiple_of(oth_col if i == 0 else own_col, 128)
        return pltpu.make_async_copy(wo_h.at[:, pl.ds(col, 1024)], wo_v.at[i, pl.ds(0, 256)], s_wo.at[i])

    def wo_rcp(i):
        col = pl.multiple_of(peer_half + ((1 - yy) if i == 0 else yy) * 1024, 128)
        return pltpu.make_async_remote_copy(
            wo_h.at[:, pl.ds(col, 1024)], wo_v.at[i, pl.ds(256, 256)],
            wo_ss, wo_rs, device_id=core_dev, device_id_type=MESH)

    barrier = pltpu.get_barrier_semaphore()
    for d in (1, 2, 3):
        pl.semaphore_signal(barrier, inc=1, device_id=seq_dev(d), device_id_type=MESH)
        pl.semaphore_signal(barrier, inc=1, device_id=z_dev(d), device_id_type=MESH)

    def load_body(c, carry):
        k_cp(c).start()
        v_cp(c).start()

        @pl.when(c == 2)
        def _():
            for i in range(2):
                wo_cp(i).start()
        return carry

    lens_cp.wait()

    sub8 = lax.broadcasted_iota(jnp.int32, (8, 128), 0)
    lane8 = lax.broadcasted_iota(jnp.int32, (8, 128), 1)

    def len_body(g, carry):
        r0 = pl.multiple_of(g * 8, 8)
        acc = jnp.zeros((8, 128), jnp.int32)
        for b in range(8):
            acc = jnp.where(sub8 == b, lens_s[r0 + b], acc)
        len_v[pl.ds(r0, 8), :] = acc
        return carry

    lax.fori_loop(0, ROWS // 8, len_body, 0)

    lane = lax.broadcasted_iota(jnp.int32, (ROWS, HD), 1)
    inv_freq = jnp.exp((lane % 64).astype(F32) * (-math.log(ROPE_THETA) / 64.0))
    angle = (len_v[...] - 1).astype(F32) * inv_freq
    cosv = jnp.cos(angle)
    sinv = jnp.where(lane < 64, -jnp.sin(angle), jnp.sin(angle))

    q_raw = jnp.zeros((ROWS, 2 * HD), F32)
    for i in range(NW):
        x_cp(i).wait()
        wq_cp(i).wait()
        if i == 2:
            lax.fori_loop(0, NC, load_body, 0)
        slot = i % 2
        wf_v[slot] = wq_v[pl.ds(i * WR, WR), :].astype(F32)
        w0 = wf_v[slot, pl.ds(0, WR // 2, 2), :].astype(BF16)
        w1 = wf_v[slot, pl.ds(1, WR // 2, 2), :].astype(BF16)
        w = jnp.concatenate([w0, w1], axis=1)
        q_raw = q_raw + jnp.dot(x_v[:, pl.ds(i * (WR // 2), WR // 2)], w, preferred_element_type=F32)
    for hh in range(2):
        qh = q_raw[:, hh * HD:(hh + 1) * HD]
        rot = pltpu.roll(qh, 64, 1)
        q_all[s, :, hh * HD:(hh + 1) * HD] = (qh * cosv + rot * sinv).astype(BF16)

    pl.semaphore_wait(barrier, 6)


    def q_cp(h, d, src):
        return pltpu.make_async_remote_copy(
            q_all.at[src, pl.ds(pl.multiple_of(h * RB, RB), RB)], q_all.at[src, pl.ds(pl.multiple_of(h * RB, RB), RB)],
            q_ss, q_rs.at[h], device_id=seq_dev(d), device_id_type=MESH)

    def send_q(h, carry):
        for d in (2, 1, 3):
            q_cp(h, d, s).start()
        return carry

    lax.fori_loop(0, QH, send_q, 0)
    for i in range(2):
        wo_rcp(i).start()

    scale = HD ** -0.5 * math.log2(math.e)
    col8 = lax.broadcasted_iota(jnp.int32, (8, 2 * T), 1)
    big = 1 << 20
    colkey = [jnp.where(col8 % 2 == n, col8 // 2, big) for n in range(2)]
    t_off = s * T
    row64 = lax.broadcasted_iota(jnp.int32, (64, HD), 0) % 8

    def o_cp(c, d):
        return pltpu.make_async_remote_copy(
            o_send.at[c, (s + d) % 4], o_recv.at[c, d - 1],
            o_ss, o_rs.at[c], device_id=seq_dev(d), device_id_type=MESH)

    def issue_scores(c):
        rows = pl.ds(c * RB, RB)
        arrived(q_all.at[pl.ds(0, 3), rows], q_rs.at[c])
        k_cp(c).wait()
        return pl.multiple_of(c * RB, RB)

    def scores(r0):
        qf = [q_all[i, pl.ds(r0, RB), :].astype(F32) for i in range(4)]
        for o in range(2):
            q64 = jnp.concatenate(
                [qf[i][8 * o:8 * o + 8, hh * HD:(hh + 1) * HD] for i in range(4) for hh in range(2)], axis=0)
            lhs = jnp.concatenate([jnp.where(row64 == b, q64, 0.0).astype(BF16) for b in range(8)], axis=1)
            kn = jnp.concatenate([k_v[r0 + 8 * o + b] for b in range(NX)], axis=1)
            res = lax.dot_general(lhs[:, :NX * HD], kn, (((1,), (1,)), ((), ())), preferred_element_type=F32)
            if NX < 8:
                kt = jnp.concatenate([k_v[r0 + 8 * o + b].T for b in range(NX, 8)], axis=0)
                res = res + jnp.dot(lhs[:, NX * HD:], kt, preferred_element_type=F32)
            s_scr[o] = res

    def softmax(c):
        r0 = pl.multiple_of(c * RB, RB)
        ml = [jnp.zeros((8, 128), F32) for _ in range(4)]
        for o in range(2):
            lim = len_v[pl.ds(r0 + 8 * o, 8), :] - t_off
            lim = jnp.concatenate([lim] * 4, axis=1)
            mask = [colkey[n] < lim for n in range(2)]
            for g2 in range(4):
                ps = []
                for g in (2 * g2, 2 * g2 + 1):
                    zz = jnp.where(mask[g // 4], s_scr[o, 8 * g:8 * g + 8, :] * scale, NEG)
                    m = jnp.maximum(jnp.max(zz, axis=1, keepdims=True), FLOOR)
                    p = jnp.exp2(zz - m)
                    l = jnp.sum(p, axis=1, keepdims=True)
                    ml[g // 2] = jnp.where(lane8 == 4 * o + g % 2, m, ml[g // 2])
                    ml[g // 2] = jnp.where(lane8 == 4 * o + 2 + g % 2, l, ml[g // 2])
                    ps.append(p)
                p_scr[o, 16 * g2:16 * g2 + 16, :] = jnp.concatenate(ps, axis=0).astype(BF16)
        for i in range(4):
            o_send[c, i, pl.ds(2 * RB, 8), :] = ml[i]

    def weighted(c):
        r0 = pl.multiple_of(c * RB, RB)
        for o in range(2):
            vc = jnp.concatenate([v_v[r0 + 8 * o + b] for b in range(8)], axis=1)
            res = jnp.dot(p_scr[o], vc, preferred_element_type=F32)
            acc = jnp.where(row64 == 0, res[:, :HD], 0.0)
            for b in range(1, 8):
                acc = jnp.where(row64 == b, res[:, b * HD:(b + 1) * HD], acc)
            for i in range(4):
                for hh in range(2):
                    g = 2 * i + hh
                    o_send[c, i, pl.ds(hh * RB + 8 * o, 8), :] = acc[8 * g:8 * g + 8]

    def send_o(c):
        for d in (2, 3, 1):
            o_cp(c, d).start()

    def attention(k):
        done = 0 if k == 0 else k - 1
        if k != 1:
            v_cp(done).wait()
        if k < NC:
            r0 = issue_scores(k)
        if k > 1:
            softmax(done)
        if k < NC:
            scores(r0)
        if k == 0:
            softmax(done)
        if k != 1:
            weighted(done)
            send_o(done)

    def a_cp(c):
        rows = pl.ds(pl.multiple_of(c * RB, RB), RB)
        return pltpu.make_async_remote_copy(
            at_own.at[rows], at_peer.at[rows], a_ss, a_rs.at[c],
            device_id=core_dev, device_id_type=MESH)

    def stage_b(c):
        arrived(o_recv.at[c], o_rs.at[c])
        mls = [o_send[c, s, pl.ds(2 * RB, 8), :]] + [o_recv[c, d, pl.ds(2 * RB, 8), :] for d in range(3)]
        mx = jnp.maximum(jnp.maximum(mls[0], mls[1]), jnp.maximum(mls[2], mls[3]))
        is_m = (lane8 % 4) < 2
        fs = [jnp.exp2(jnp.where(is_m, v - mx, 0.0)) for v in mls]
        tot = sum(f * pltpu.roll(v, 126, 1) for f, v in zip(fs, mls))
        tot = jnp.where(is_m, tot, 1.0)
        gs = [f / tot for f in fs]
        r0 = pl.multiple_of(c * RB, RB)
        for hh in range(2):
            parts = []
            for o in range(2):
                idx = 4 * o + hh
                rows = pl.ds(hh * RB + 8 * o, 8)
                acc = jnp.broadcast_to(gs[0][:, idx:idx + 1], (8, HD)) * o_send[c, s, rows, :]
                for d in range(3):
                    acc = acc + jnp.broadcast_to(gs[d + 1][:, idx:idx + 1], (8, HD)) * o_recv[c, d, rows, :]
                parts.append(acc)
            at_own[pl.ds(r0, RB), hh * HD:(hh + 1) * HD] = jnp.concatenate(parts, axis=0).astype(BF16)
        a_cp(c).start()

    def y_cp(c):
        return pltpu.make_async_remote_copy(
            y_send.at[c], y_recv.at[c], y_ss, y_rs.at[c], device_id=y_dev, device_id_type=MESH)

    def stage_c(c):
        if c == 0:
            for i in range(2):
                wo_cp(i).wait()
            arrived(wo_v.at[:, pl.ds(256, 256)], wo_rs)
        a_cp(c).wait_recv()
        r0 = pl.multiple_of(c * RB, RB)
        at = jnp.concatenate([at_own[pl.ds(r0, RB), :], at_peer[pl.ds(r0, RB), :]], axis=1)
        if c in Z_FIRST:
            for p in range(2):
                part = jnp.dot(at, wo_v[p], preferred_element_type=F32)
                for i in range(4):
                    f_buf[slot_f(c), i, p] = part[:, i * 256:(i + 1) * 256]
            for d in (2, 1, 3):
                f_cp(c, d).start()
            return
        y_send[c] = jnp.dot(at, wo_v[0], preferred_element_type=F32)
        y_cp(c).start()
        y_keep[c] = jnp.dot(at, wo_v[1], preferred_element_type=F32)

    def slot_f(c):
        return Z_FIRST.index(c)

    def f_cp(c, d):
        i = slot_f(c)
        return pltpu.make_async_remote_copy(
            f_buf.at[i, (z + d) % 4], f_recv.at[i, d - 1],
            f_ss, z_rs.at[c], device_id=z_dev(d), device_id_type=MESH)

    def g_cp(c):
        i = slot_f(c)
        return pltpu.make_async_remote_copy(
            g_buf.at[i, 0], g_recv.at[i], g_ss, y_rs.at[c], device_id=y_dev, device_id_type=MESH)

    def z_cp(c, d):
        return pltpu.make_async_remote_copy(
            z_buf.at[c, (z + d) % 4], z_recv.at[c, d - 1],
            z_ss, z_rs.at[c], device_id=z_dev(d), device_id_type=MESH)

    def stage_d(c):
        if c in Z_FIRST:
            i = slot_f(c)
            arrived(f_recv.at[i], z_rs.at[c])
            g_buf[i] = (f_buf[i, z] + f_recv[i, 0]) + (f_recv[i, 1] + f_recv[i, 2])
            g_cp(c).start()
            return
        y_cp(c).wait_recv()
        tot = y_keep[c] + y_recv[c]
        for i in range(4):
            z_buf[c, i] = tot[:, i * 256:(i + 1) * 256]
        for d in (2, 1, 3):
            z_cp(c, d).start()

    def ez_cp(c, d, src):
        rows = pl.ds(pl.multiple_of(c * RB, RB), RB)
        cols = pl.ds(pl.multiple_of(own_col + src * 256, 128), 256)
        return pltpu.make_async_remote_copy(
            out_v.at[rows, cols], out_v.at[rows, cols],
            ez_ss, ez_rs.at[c], device_id=z_dev(d), device_id_type=MESH)

    def stage_e(c):
        if c in Z_FIRST:
            arrived(g_recv.at[slot_f(c)], y_rs.at[c])
        else:
            arrived(z_recv.at[c], z_rs.at[c])
        r0 = pl.multiple_of(c * RB, RB)
        cols = pl.ds(pl.multiple_of(own_col + z * 256, 128), 256)
        if c in Z_FIRST:
            tot = g_buf[slot_f(c), 1] + g_recv[slot_f(c)]
        else:
            tot = (z_buf[c, z] + z_recv[c, 0]) + (z_recv[c, 1] + z_recv[c, 2])
        out_v[pl.ds(r0, RB), cols] = (x_v[pl.ds(r0, RB), cols].astype(F32) + tot).astype(BF16)
        for d in (2, 1, 3):
            ez_cp(c, d, z).start()

    def quarter(c, col):
        return out_v.at[pl.ds(pl.multiple_of(c * RB, RB), RB), pl.ds(pl.multiple_of(col, 128), 1024)]

    def ey_cp(c, col):
        q = quarter(c, col)
        return pltpu.make_async_remote_copy(q, q, ey_ss, ey_rs.at[c], device_id=y_dev, device_id_type=MESH)

    def ec_cp(c, col):
        q = quarter(c, col)
        return pltpu.make_async_remote_copy(q, q, ec_ss, ec_rs.at[c], device_id=core_dev, device_id_type=MESH)

    def ed_cp(c, col):
        q = quarter(c, col)
        return pltpu.make_async_remote_copy(q, q, ed_ss, ed_rs.at[c], device_id=core_dev, device_id_type=MESH)

    def stage_f(c):
        arrived(out_v.at[pl.ds(c * RB, RB), pl.ds(0, 768)], ez_rs.at[c])
        ey_cp(c, own_col).start()
        ec_cp(c, own_col).start()

    def stage_g(c):
        ey_cp(c, oth_col).wait_recv()
        ed_cp(c, oth_col).start()

    def stage_h(c):
        ec_cp(c, peer_half + yy * 1024).wait_recv()
        ed_cp(c, peer_half + (1 - yy) * 1024).wait_recv()

    stages = (attention, stage_b, stage_c, stage_d, stage_e, stage_f, stage_g, stage_h)
    for stage, c in ORDER:
        stages[stage](c)

    sent(q_all.at[pl.ds(0, 3)], q_ss)
    sent(wo_v.at[:, pl.ds(0, 256)], wo_ss)
    sent(o_recv, o_ss)
    sent(at_own, a_ss)
    sent(y_send.at[pl.ds(0, NC - NF)], y_ss)
    sent(z_recv.at[pl.ds(0, NC - NF)], z_ss)
    sent(f_recv, f_ss)
    sent(g_recv, g_ss)
    sent(out_v.at[:, pl.ds(0, 768)], ez_ss)
    for sem in (ey_ss, ec_ss, ed_ss):
        sent(out_v.at[:, pl.ds(0, 1024)], sem)


def solution(mesh):
    def local_step(x_hidden, seq_lens, k_loc, v_loc, wq_loc, wo_loc):
        k2 = k_loc.reshape(ROWS, 2 * T, HD)
        v2 = v_loc.reshape(ROWS, 2 * T, HD)
        wq2 = wq_loc.reshape(2 * D, HD)
        wo2 = wo_loc.reshape(2 * HD, D)
        dma = pltpu.SemaphoreType.DMA
        any_spec = pl.BlockSpec(memory_space=pltpu.HBM)
        return pl.pallas_call(
            kernel,
            out_shape=jax.ShapeDtypeStruct((ROWS, D), BF16),
            in_specs=[any_spec] * 6,
            out_specs=pl.BlockSpec(memory_space=pltpu.VMEM),
            scratch_shapes=[
                pltpu.SMEM((ROWS,), jnp.int32),
                pltpu.VMEM((ROWS, D), BF16),
                pltpu.VMEM((ROWS, 2 * T, HD), BF16),
                pltpu.VMEM((ROWS, 2 * T, HD), BF16),
                pltpu.VMEM((2 * D, HD), BF16),
                pltpu.VMEM((2, WR, HD), F32),
                pltpu.VMEM((2, 512, 1024), BF16),
                pltpu.VMEM((ROWS, 128), jnp.int32),
                pltpu.VMEM((4, ROWS, 2 * HD), BF16),
                pltpu.VMEM((NC, 4, OR_, HD), F32),
                pltpu.VMEM((NC, 3, OR_, HD), F32),
                pltpu.VMEM((ROWS, 2 * HD), BF16),
                pltpu.VMEM((ROWS, 2 * HD), BF16),
                pltpu.VMEM((NC, RB, 1024), F32),
                pltpu.VMEM((NC, RB, 1024), F32),
                pltpu.VMEM((NC, RB, 1024), F32),
                pltpu.VMEM((NC, 4, RB, 256), F32),
                pltpu.VMEM((NC, 3, RB, 256), F32),
                pltpu.VMEM((NF, 4, 2, RB, 256), F32),
                pltpu.VMEM((NF, 3, 2, RB, 256), F32),
                pltpu.VMEM((NF, 2, RB, 256), F32),
                pltpu.VMEM((NF, RB, 256), F32),
                pltpu.VMEM((2, 64, 2 * T), F32),
                pltpu.VMEM((2, 64, 2 * T), BF16),
                dma(()), dma((NW,)), dma((NW,)), dma((NC,)), dma((NC,)), dma((2,)),
                dma(()), dma(()),
                dma(()), dma((NC,)),
                dma(()), dma((NC,)),
                dma(()), dma((NC,)),
                dma(()), dma((NC,)),
                dma(()), dma((NC,)),
                dma(()), dma(()),
                dma(()), dma((NC,)),
                dma(()), dma((NC,)),
                dma(()), dma((NC,)),
                dma(()), dma((NC,)),
            ],
            compiler_params=pltpu.CompilerParams(
                collective_id=0, has_side_effects=True, vmem_limit_bytes=52 * 1024 * 1024),
            name="decode",
        )(seq_lens, x_hidden, k2, v2, wq2, wo2)

    return jax.shard_map(
        local_step,
        mesh=mesh,
        in_specs=(P('dp', None), P('dp'), P('dp', 'seq', 'kvh', None), P('dp', 'seq', 'kvh', None),
                  P(None, ('kvh', 'seq'), None), P(('kvh', 'seq'), None, None)),
        out_specs=P('dp', None),
        check_vma=False)
```

```python
import math

import jax
import jax.numpy as jnp
from jax import lax
from jax.experimental import pallas as pl
from jax.experimental.pallas import tpu as pltpu
from jax.sharding import PartitionSpec as P

ROPE_THETA = 500000.0
NEG = -1e30
FLOOR = -1e29
F32 = jnp.float32
BF16 = jnp.bfloat16
MESH = pl.DeviceIdType.MESH

ROWS = 128
RB = 16
NC = ROWS // RB
T = 256
D = 4096
HD = 128
NW = 4
WR = 2 * D // NW
QH = NC
NX = 3
OR_ = 2 * RB + 8

Z_FIRST = (0, 1, 2)
NF = len(Z_FIRST)

ORDER = (
    (0, 0), (0, 1), (0, 2), (0, 3), (0, 4), (1, 0), (0, 5), (1, 1), (2, 0), (0, 6), (0, 7), (1, 3), (2, 1),
    (0, 8), (1, 4), (1, 2), (2, 3), (2, 2), (1, 6), (2, 4), (1, 5), (1, 7), (3, 3), (3, 0), (2, 5), (2, 6),
    (3, 1), (2, 7), (3, 4), (4, 0), (3, 5), (4, 1), (3, 2), (3, 6), (3, 7), (4, 2), (4, 3), (4, 5), (5, 1),
    (4, 4), (4, 6), (5, 0), (4, 7), (5, 2), (5, 3), (5, 5), (6, 1), (5, 4), (5, 6), (5, 7), (6, 5), (6, 2),
    (6, 4), (6, 6), (7, 2), (6, 3), (7, 1), (6, 0), (6, 7), (7, 5), (7, 4), (7, 3), (7, 0), (7, 6), (7, 7),
)


def kernel(lens_h, x_h, k_h, v_h, wq_h, wo_h, out_v,
           lens_s, x_v, k_v, v_v, wq_v, wf_v, wo_v, len_v, q_all,
           o_send, o_recv, at_own, at_peer, y_keep, y_send, y_recv,
           z_buf, z_recv, f_buf, f_recv, g_buf, g_recv, s_scr, p_scr,
           s_len, s_x, s_wq, s_k, s_v, s_wo,
           wo_ss, wo_rs, q_ss, q_rs, o_ss, o_rs, a_ss, a_rs, y_ss, y_rs,
           z_ss, z_rs, f_ss, g_ss, ez_ss, ez_rs, ey_ss, ey_rs, ec_ss, ec_rs, ed_ss, ed_rs):
    dp = lax.axis_index("dp")
    z = lax.axis_index("kvh")
    s = lax.axis_index("seq")
    yy = s // 2
    cc = s % 2
    half_c = cc * 2048
    own_col = half_c + yy * 1024
    oth_col = half_c + (1 - yy) * 1024
    peer_half = (1 - cc) * 2048

    def seq_dev(d):
        return (dp, z, (s + d) % 4)

    def z_dev(d):
        return (dp, (z + d) % 4, s)

    def arrived(ref, sem):
        pltpu.make_async_remote_copy(ref, ref, sem, sem, device_id=seq_dev(1), device_id_type=MESH).wait_recv()

    def sent(ref, sem):
        pltpu.make_async_remote_copy(ref, ref, sem, sem, device_id=seq_dev(1), device_id_type=MESH).wait_send()

    core_dev = (dp, z, yy * 2 + (1 - cc))
    y_dev = (dp, z, (1 - yy) * 2 + cc)

    def x_cp(i):
        cols = pl.ds(i * (WR // 2), WR // 2)
        return pltpu.make_async_copy(x_h.at[:, cols], x_v.at[:, cols], s_x.at[i])

    lens_cp = pltpu.make_async_copy(lens_h, lens_s, s_len)
    lens_cp.start()

    def wq_cp(i):
        return pltpu.make_async_copy(wq_h.at[pl.ds(i * WR, WR)], wq_v.at[pl.ds(i * WR, WR)], s_wq.at[i])

    def load_q(i, carry):
        cols = pl.ds(pl.multiple_of(i * (WR // 2), WR // 2), WR // 2)
        rows = pl.ds(pl.multiple_of(i * WR, WR), WR)
        pltpu.make_async_copy(x_h.at[:, cols], x_v.at[:, cols], s_x.at[i]).start()
        pltpu.make_async_copy(wq_h.at[rows], wq_v.at[rows], s_wq.at[i]).start()
        return carry

    lax.fori_loop(0, NW, load_q, 0)

    def k_cp(c):
        return pltpu.make_async_copy(k_h.at[pl.ds(c * RB, RB)], k_v.at[pl.ds(c * RB, RB)], s_k.at[c])

    def v_cp(c):
        return pltpu.make_async_copy(v_h.at[pl.ds(c * RB, RB)], v_v.at[pl.ds(c * RB, RB)], s_v.at[c])

    def wo_cp(i):
        col = pl.multiple_of(oth_col if i == 0 else own_col, 128)
        return pltpu.make_async_copy(wo_h.at[:, pl.ds(col, 1024)], wo_v.at[i, pl.ds(0, 256)], s_wo.at[i])

    def wo_rcp(i):
        col = pl.multiple_of(peer_half + ((1 - yy) if i == 0 else yy) * 1024, 128)
        return pltpu.make_async_remote_copy(
            wo_h.at[:, pl.ds(col, 1024)], wo_v.at[i, pl.ds(256, 256)],
            wo_ss, wo_rs, device_id=core_dev, device_id_type=MESH)

    barrier = pltpu.get_barrier_semaphore()
    for d in (1, 2, 3):
        pl.semaphore_signal(barrier, inc=1, device_id=seq_dev(d), device_id_type=MESH)
        pl.semaphore_signal(barrier, inc=1, device_id=z_dev(d), device_id_type=MESH)

    def load_body(c, carry):
        k_cp(c).start()
        v_cp(c).start()

        @pl.when(c == 2)
        def _():
            for i in range(2):
                wo_cp(i).start()
        return carry

    lens_cp.wait()

    sub8 = lax.broadcasted_iota(jnp.int32, (8, 128), 0)
    lane8 = lax.broadcasted_iota(jnp.int32, (8, 128), 1)

    def len_body(g, carry):
        r0 = pl.multiple_of(g * 8, 8)
        acc = jnp.zeros((8, 128), jnp.int32)
        for b in range(8):
            acc = jnp.where(sub8 == b, lens_s[r0 + b], acc)
        len_v[pl.ds(r0, 8), :] = acc
        return carry

    lax.fori_loop(0, ROWS // 8, len_body, 0)

    lane = lax.broadcasted_iota(jnp.int32, (ROWS, HD), 1)
    inv_freq = jnp.exp((lane % 64).astype(F32) * (-math.log(ROPE_THETA) / 64.0))
    angle = (len_v[...] - 1).astype(F32) * inv_freq
    cosv = jnp.cos(angle)
    sinv = jnp.where(lane < 64, -jnp.sin(angle), jnp.sin(angle))

    q_raw = jnp.zeros((ROWS, 2 * HD), F32)
    for i in range(NW):
        x_cp(i).wait()
        wq_cp(i).wait()
        if i == 1:
            lax.fori_loop(0, NC, load_body, 0)
        slot = i % 2
        wf_v[slot] = wq_v[pl.ds(i * WR, WR), :].astype(F32)
        w0 = wf_v[slot, pl.ds(0, WR // 2, 2), :].astype(BF16)
        w1 = wf_v[slot, pl.ds(1, WR // 2, 2), :].astype(BF16)
        w = jnp.concatenate([w0, w1], axis=1)
        q_raw = q_raw + jnp.dot(x_v[:, pl.ds(i * (WR // 2), WR // 2)], w, preferred_element_type=F32)
    for hh in range(2):
        qh = q_raw[:, hh * HD:(hh + 1) * HD]
        rot = pltpu.roll(qh, 64, 1)
        q_all[s, :, hh * HD:(hh + 1) * HD] = (qh * cosv + rot * sinv).astype(BF16)

    pl.semaphore_wait(barrier, 6)


    def q_cp(h, d, src):
        return pltpu.make_async_remote_copy(
            q_all.at[src, pl.ds(pl.multiple_of(h * RB, RB), RB)], q_all.at[src, pl.ds(pl.multiple_of(h * RB, RB), RB)],
            q_ss, q_rs.at[h], device_id=seq_dev(d), device_id_type=MESH)

    def send_q(h, carry):
        for d in (2, 1, 3):
            q_cp(h, d, s).start()
        return carry

    lax.fori_loop(0, QH, send_q, 0)
    for i in range(2):
        wo_rcp(i).start()

    scale = HD ** -0.5 * math.log2(math.e)
    col8 = lax.broadcasted_iota(jnp.int32, (8, 2 * T), 1)
    big = 1 << 20
    colkey = [jnp.where(col8 % 2 == n, col8 // 2, big) for n in range(2)]
    t_off = s * T
    row64 = lax.broadcasted_iota(jnp.int32, (64, HD), 0) % 8

    def o_cp(c, d):
        return pltpu.make_async_remote_copy(
            o_send.at[c, (s + d) % 4], o_recv.at[c, d - 1],
            o_ss, o_rs.at[c], device_id=seq_dev(d), device_id_type=MESH)

    def issue_scores(c):
        rows = pl.ds(c * RB, RB)
        arrived(q_all.at[pl.ds(0, 3), rows], q_rs.at[c])
        k_cp(c).wait()
        return pl.multiple_of(c * RB, RB)

    def scores(r0):
        qf = [q_all[i, pl.ds(r0, RB), :].astype(F32) for i in range(4)]
        for o in range(2):
            q64 = jnp.concatenate(
                [qf[i][8 * o:8 * o + 8, hh * HD:(hh + 1) * HD] for i in range(4) for hh in range(2)], axis=0)
            lhs = jnp.concatenate([jnp.where(row64 == b, q64, 0.0).astype(BF16) for b in range(8)], axis=1)
            kn = jnp.concatenate([k_v[r0 + 8 * o + b] for b in range(NX)], axis=1)
            res = lax.dot_general(lhs[:, :NX * HD], kn, (((1,), (1,)), ((), ())), preferred_element_type=F32)
            if NX < 8:
                kt = jnp.concatenate([k_v[r0 + 8 * o + b].T for b in range(NX, 8)], axis=0)
                res = res + jnp.dot(lhs[:, NX * HD:], kt, preferred_element_type=F32)
            s_scr[o] = res

    def softmax(c):
        r0 = pl.multiple_of(c * RB, RB)
        ml = [jnp.zeros((8, 128), F32) for _ in range(4)]
        for o in range(2):
            lim = len_v[pl.ds(r0 + 8 * o, 8), :] - t_off
            lim = jnp.concatenate([lim] * 4, axis=1)
            mask = [colkey[n] < lim for n in range(2)]
            for g2 in range(4):
                ps = []
                for g in (2 * g2, 2 * g2 + 1):
                    zz = jnp.where(mask[g // 4], s_scr[o, 8 * g:8 * g + 8, :] * scale, NEG)
                    m = jnp.maximum(jnp.max(zz, axis=1, keepdims=True), FLOOR)
                    p = jnp.exp2(zz - m)
                    l = jnp.sum(p, axis=1, keepdims=True)
                    ml[g // 2] = jnp.where(lane8 == 4 * o + g % 2, m, ml[g // 2])
                    ml[g // 2] = jnp.where(lane8 == 4 * o + 2 + g % 2, l, ml[g // 2])
                    ps.append(p)
                p_scr[o, 16 * g2:16 * g2 + 16, :] = jnp.concatenate(ps, axis=0).astype(BF16)
        for i in range(4):
            o_send[c, i, pl.ds(2 * RB, 8), :] = ml[i]

    def weighted(c):
        r0 = pl.multiple_of(c * RB, RB)
        for o in range(2):
            vc = jnp.concatenate([v_v[r0 + 8 * o + b] for b in range(8)], axis=1)
            res = jnp.dot(p_scr[o], vc, preferred_element_type=F32)
            acc = jnp.where(row64 == 0, res[:, :HD], 0.0)
            for b in range(1, 8):
                acc = jnp.where(row64 == b, res[:, b * HD:(b + 1) * HD], acc)
            for i in range(4):
                for hh in range(2):
                    g = 2 * i + hh
                    o_send[c, i, pl.ds(hh * RB + 8 * o, 8), :] = acc[8 * g:8 * g + 8]

    def send_o(c):
        for d in (2, 3, 1):
            o_cp(c, d).start()

    def attention(k):
        done = 0 if k == 0 else k - 1
        if k != 1:
            v_cp(done).wait()
        if k < NC:
            r0 = issue_scores(k)
        if k > 1:
            softmax(done)
        if k < NC:
            scores(r0)
        if k == 0:
            softmax(done)
        if k != 1:
            weighted(done)
            send_o(done)

    def a_cp(c):
        rows = pl.ds(pl.multiple_of(c * RB, RB), RB)
        return pltpu.make_async_remote_copy(
            at_own.at[rows], at_peer.at[rows], a_ss, a_rs.at[c],
            device_id=core_dev, device_id_type=MESH)

    def stage_b(c):
        arrived(o_recv.at[c], o_rs.at[c])
        mls = [o_send[c, s, pl.ds(2 * RB, 8), :]] + [o_recv[c, d, pl.ds(2 * RB, 8), :] for d in range(3)]
        mx = jnp.maximum(jnp.maximum(mls[0], mls[1]), jnp.maximum(mls[2], mls[3]))
        is_m = (lane8 % 4) < 2
        fs = [jnp.exp2(jnp.where(is_m, v - mx, 0.0)) for v in mls]
        tot = sum(f * pltpu.roll(v, 126, 1) for f, v in zip(fs, mls))
        tot = jnp.where(is_m, tot, 1.0)
        gs = [f / tot for f in fs]
        r0 = pl.multiple_of(c * RB, RB)
        for hh in range(2):
            parts = []
            for o in range(2):
                idx = 4 * o + hh
                rows = pl.ds(hh * RB + 8 * o, 8)
                acc = jnp.broadcast_to(gs[0][:, idx:idx + 1], (8, HD)) * o_send[c, s, rows, :]
                for d in range(3):
                    acc = acc + jnp.broadcast_to(gs[d + 1][:, idx:idx + 1], (8, HD)) * o_recv[c, d, rows, :]
                parts.append(acc)
            at_own[pl.ds(r0, RB), hh * HD:(hh + 1) * HD] = jnp.concatenate(parts, axis=0).astype(BF16)
        a_cp(c).start()

    def y_cp(c):
        return pltpu.make_async_remote_copy(
            y_send.at[c], y_recv.at[c], y_ss, y_rs.at[c], device_id=y_dev, device_id_type=MESH)

    def stage_c(c):
        if c == 0:
            for i in range(2):
                wo_cp(i).wait()
            arrived(wo_v.at[:, pl.ds(256, 256)], wo_rs)
        a_cp(c).wait_recv()
        r0 = pl.multiple_of(c * RB, RB)
        at = jnp.concatenate([at_own[pl.ds(r0, RB), :], at_peer[pl.ds(r0, RB), :]], axis=1)
        if c in Z_FIRST:
            for p in range(2):
                part = jnp.dot(at, wo_v[p], preferred_element_type=F32)
                for i in range(4):
                    f_buf[slot_f(c), i, p] = part[:, i * 256:(i + 1) * 256]
            for d in (2, 1, 3):
                f_cp(c, d).start()
            return
        y_send[c] = jnp.dot(at, wo_v[0], preferred_element_type=F32)
        y_cp(c).start()
        y_keep[c] = jnp.dot(at, wo_v[1], preferred_element_type=F32)

    def slot_f(c):
        return Z_FIRST.index(c)

    def f_cp(c, d):
        i = slot_f(c)
        return pltpu.make_async_remote_copy(
            f_buf.at[i, (z + d) % 4], f_recv.at[i, d - 1],
            f_ss, z_rs.at[c], device_id=z_dev(d), device_id_type=MESH)

    def g_cp(c):
        i = slot_f(c)
        return pltpu.make_async_remote_copy(
            g_buf.at[i, 0], g_recv.at[i], g_ss, y_rs.at[c], device_id=y_dev, device_id_type=MESH)

    def z_cp(c, d):
        return pltpu.make_async_remote_copy(
            z_buf.at[c, (z + d) % 4], z_recv.at[c, d - 1],
            z_ss, z_rs.at[c], device_id=z_dev(d), device_id_type=MESH)

    def stage_d(c):
        if c in Z_FIRST:
            i = slot_f(c)
            arrived(f_recv.at[i], z_rs.at[c])
            g_buf[i] = (f_buf[i, z] + f_recv[i, 0]) + (f_recv[i, 1] + f_recv[i, 2])
            g_cp(c).start()
            return
        y_cp(c).wait_recv()
        tot = y_keep[c] + y_recv[c]
        for i in range(4):
            z_buf[c, i] = tot[:, i * 256:(i + 1) * 256]
        for d in (2, 1, 3):
            z_cp(c, d).start()

    def ez_cp(c, d, src):
        rows = pl.ds(pl.multiple_of(c * RB, RB), RB)
        cols = pl.ds(pl.multiple_of(own_col + src * 256, 128), 256)
        return pltpu.make_async_remote_copy(
            out_v.at[rows, cols], out_v.at[rows, cols],
            ez_ss, ez_rs.at[c], device_id=z_dev(d), device_id_type=MESH)

    def stage_e(c):
        if c in Z_FIRST:
            arrived(g_recv.at[slot_f(c)], y_rs.at[c])
        else:
            arrived(z_recv.at[c], z_rs.at[c])
        r0 = pl.multiple_of(c * RB, RB)
        cols = pl.ds(pl.multiple_of(own_col + z * 256, 128), 256)
        if c in Z_FIRST:
            tot = g_buf[slot_f(c), 1] + g_recv[slot_f(c)]
        else:
            tot = (z_buf[c, z] + z_recv[c, 0]) + (z_recv[c, 1] + z_recv[c, 2])
        out_v[pl.ds(r0, RB), cols] = (x_v[pl.ds(r0, RB), cols].astype(F32) + tot).astype(BF16)
        for d in (2, 1, 3):
            ez_cp(c, d, z).start()

    def quarter(c, col):
        return out_v.at[pl.ds(pl.multiple_of(c * RB, RB), RB), pl.ds(pl.multiple_of(col, 128), 1024)]

    def ey_cp(c, col):
        q = quarter(c, col)
        return pltpu.make_async_remote_copy(q, q, ey_ss, ey_rs.at[c], device_id=y_dev, device_id_type=MESH)

    def ec_cp(c, col):
        q = quarter(c, col)
        return pltpu.make_async_remote_copy(q, q, ec_ss, ec_rs.at[c], device_id=core_dev, device_id_type=MESH)

    def ed_cp(c, col):
        q = quarter(c, col)
        return pltpu.make_async_remote_copy(q, q, ed_ss, ed_rs.at[c], device_id=core_dev, device_id_type=MESH)

    def stage_f(c):
        arrived(out_v.at[pl.ds(c * RB, RB), pl.ds(0, 768)], ez_rs.at[c])
        ey_cp(c, own_col).start()
        ec_cp(c, own_col).start()

    def stage_g(c):
        ey_cp(c, oth_col).wait_recv()
        ed_cp(c, oth_col).start()

    def stage_h(c):
        ec_cp(c, peer_half + yy * 1024).wait_recv()
        ed_cp(c, peer_half + (1 - yy) * 1024).wait_recv()

    stages = (attention, stage_b, stage_c, stage_d, stage_e, stage_f, stage_g, stage_h)
    for stage, c in ORDER:
        stages[stage](c)

    sent(q_all.at[pl.ds(0, 3)], q_ss)
    sent(wo_v.at[:, pl.ds(0, 256)], wo_ss)
    sent(o_recv, o_ss)
    sent(at_own, a_ss)
    sent(y_send.at[pl.ds(0, NC - NF)], y_ss)
    sent(z_recv.at[pl.ds(0, NC - NF)], z_ss)
    sent(f_recv, f_ss)
    sent(g_recv, g_ss)
    sent(out_v.at[:, pl.ds(0, 768)], ez_ss)
    for sem in (ey_ss, ec_ss, ed_ss):
        sent(out_v.at[:, pl.ds(0, 1024)], sem)


def solution(mesh):
    def local_step(x_hidden, seq_lens, k_loc, v_loc, wq_loc, wo_loc):
        k2 = k_loc.reshape(ROWS, 2 * T, HD)
        v2 = v_loc.reshape(ROWS, 2 * T, HD)
        wq2 = wq_loc.reshape(2 * D, HD)
        wo2 = wo_loc.reshape(2 * HD, D)
        dma = pltpu.SemaphoreType.DMA
        any_spec = pl.BlockSpec(memory_space=pltpu.HBM)
        return pl.pallas_call(
            kernel,
            out_shape=jax.ShapeDtypeStruct((ROWS, D), BF16),
            in_specs=[any_spec] * 6,
            out_specs=pl.BlockSpec(memory_space=pltpu.VMEM),
            scratch_shapes=[
                pltpu.SMEM((ROWS,), jnp.int32),
                pltpu.VMEM((ROWS, D), BF16),
                pltpu.VMEM((ROWS, 2 * T, HD), BF16),
                pltpu.VMEM((ROWS, 2 * T, HD), BF16),
                pltpu.VMEM((2 * D, HD), BF16),
                pltpu.VMEM((2, WR, HD), F32),
                pltpu.VMEM((2, 512, 1024), BF16),
                pltpu.VMEM((ROWS, 128), jnp.int32),
                pltpu.VMEM((4, ROWS, 2 * HD), BF16),
                pltpu.VMEM((NC, 4, OR_, HD), F32),
                pltpu.VMEM((NC, 3, OR_, HD), F32),
                pltpu.VMEM((ROWS, 2 * HD), BF16),
                pltpu.VMEM((ROWS, 2 * HD), BF16),
                pltpu.VMEM((NC, RB, 1024), F32),
                pltpu.VMEM((NC, RB, 1024), F32),
                pltpu.VMEM((NC, RB, 1024), F32),
                pltpu.VMEM((NC, 4, RB, 256), F32),
                pltpu.VMEM((NC, 3, RB, 256), F32),
                pltpu.VMEM((NF, 4, 2, RB, 256), F32),
                pltpu.VMEM((NF, 3, 2, RB, 256), F32),
                pltpu.VMEM((NF, 2, RB, 256), F32),
                pltpu.VMEM((NF, RB, 256), F32),
                pltpu.VMEM((2, 64, 2 * T), F32),
                pltpu.VMEM((2, 64, 2 * T), BF16),
                dma(()), dma((NW,)), dma((NW,)), dma((NC,)), dma((NC,)), dma((2,)),
                dma(()), dma(()),
                dma(()), dma((NC,)),
                dma(()), dma((NC,)),
                dma(()), dma((NC,)),
                dma(()), dma((NC,)),
                dma(()), dma((NC,)),
                dma(()), dma(()),
                dma(()), dma((NC,)),
                dma(()), dma((NC,)),
                dma(()), dma((NC,)),
                dma(()), dma((NC,)),
            ],
            compiler_params=pltpu.CompilerParams(
                collective_id=0, has_side_effects=True, vmem_limit_bytes=52 * 1024 * 1024),
            name="decode",
        )(seq_lens, x_hidden, k2, v2, wq2, wo2)

    return jax.shard_map(
        local_step,
        mesh=mesh,
        in_specs=(P('dp', None), P('dp'), P('dp', 'seq', 'kvh', None), P('dp', 'seq', 'kvh', None),
                  P(None, ('kvh', 'seq'), None), P(('kvh', 'seq'), None, None)),
        out_specs=P('dp', None),
        check_vma=False)
```

```python
import math

import jax
import jax.numpy as jnp
from jax import lax
from jax.experimental import pallas as pl
from jax.experimental.pallas import tpu as pltpu
from jax.sharding import PartitionSpec as P

ROPE_THETA = 500000.0
NEG = -1e30
FLOOR = -1e29
F32 = jnp.float32
BF16 = jnp.bfloat16
MESH = pl.DeviceIdType.MESH

ROWS = 128
RB = 16
NC = ROWS // RB
T = 256
D = 4096
HD = 128
NW = 4
WR = 2 * D // NW
QH = NC
NX = 3
OR_ = 2 * RB + 8

Z_FIRST = (0, 1, 2)
NF = len(Z_FIRST)

ORDER = (
    (0, 0), (0, 1), (0, 2), (0, 3), (1, 0), (0, 4), (2, 0), (1, 1), (0, 5), (0, 6), (2, 1), (1, 3), (0, 7),
    (1, 4), (2, 3), (1, 2), (0, 8), (2, 2), (2, 4), (1, 5), (1, 6), (2, 5), (3, 0), (3, 3), (3, 1), (2, 6),
    (1, 7), (3, 4), (2, 7), (3, 5), (4, 0), (4, 3), (3, 6), (4, 1), (3, 7), (3, 2), (4, 2), (4, 4), (5, 3),
    (4, 5), (4, 6), (5, 0), (5, 1), (4, 7), (6, 0), (5, 4), (6, 3), (5, 2), (6, 1), (5, 5), (5, 6), (5, 7),
    (6, 5), (6, 4), (6, 6), (6, 2), (6, 7), (7, 2), (7, 0), (7, 5), (7, 6), (7, 1), (7, 3), (7, 4), (7, 7),
)


def kernel(lens_h, x_h, k_h, v_h, wq_h, wo_h, out_v,
           lens_s, x_v, k_v, v_v, wq_v, wf_v, wo_v, len_v, q_all,
           o_send, o_recv, at_own, at_peer, y_keep, y_send, y_recv,
           z_buf, z_recv, f_buf, f_recv, g_buf, g_recv, s_scr, p_scr,
           s_len, s_x, s_wq, s_k, s_v, s_wo,
           wo_ss, wo_rs, q_ss, q_rs, o_ss, o_rs, a_ss, a_rs, y_ss, y_rs,
           z_ss, z_rs, f_ss, g_ss, ez_ss, ez_rs, ey_ss, ey_rs, ec_ss, ec_rs, ed_ss, ed_rs):
    dp = lax.axis_index("dp")
    z = lax.axis_index("kvh")
    s = lax.axis_index("seq")
    yy = s // 2
    cc = s % 2
    half_c = cc * 2048
    own_col = half_c + yy * 1024
    oth_col = half_c + (1 - yy) * 1024
    peer_half = (1 - cc) * 2048

    def seq_dev(d):
        return (dp, z, (s + d) % 4)

    def z_dev(d):
        return (dp, (z + d) % 4, s)

    def arrived(ref, sem):
        pltpu.make_async_remote_copy(ref, ref, sem, sem, device_id=seq_dev(1), device_id_type=MESH).wait_recv()

    def sent(ref, sem):
        pltpu.make_async_remote_copy(ref, ref, sem, sem, device_id=seq_dev(1), device_id_type=MESH).wait_send()

    core_dev = (dp, z, yy * 2 + (1 - cc))
    y_dev = (dp, z, (1 - yy) * 2 + cc)

    def x_cp(i):
        cols = pl.ds(i * (WR // 2), WR // 2)
        return pltpu.make_async_copy(x_h.at[:, cols], x_v.at[:, cols], s_x.at[i])

    lens_cp = pltpu.make_async_copy(lens_h, lens_s, s_len)
    lens_cp.start()

    def wq_cp(i):
        return pltpu.make_async_copy(wq_h.at[pl.ds(i * WR, WR)], wq_v.at[pl.ds(i * WR, WR)], s_wq.at[i])

    def load_q(i, carry):
        cols = pl.ds(pl.multiple_of(i * (WR // 2), WR // 2), WR // 2)
        rows = pl.ds(pl.multiple_of(i * WR, WR), WR)
        pltpu.make_async_copy(x_h.at[:, cols], x_v.at[:, cols], s_x.at[i]).start()
        pltpu.make_async_copy(wq_h.at[rows], wq_v.at[rows], s_wq.at[i]).start()
        return carry

    lax.fori_loop(0, NW, load_q, 0)

    def k_cp(c):
        return pltpu.make_async_copy(k_h.at[pl.ds(c * RB, RB)], k_v.at[pl.ds(c * RB, RB)], s_k.at[c])

    def v_cp(c):
        return pltpu.make_async_copy(v_h.at[pl.ds(c * RB, RB)], v_v.at[pl.ds(c * RB, RB)], s_v.at[c])

    def wo_cp(i):
        col = pl.multiple_of(oth_col if i == 0 else own_col, 128)
        return pltpu.make_async_copy(wo_h.at[:, pl.ds(col, 1024)], wo_v.at[i, pl.ds(0, 256)], s_wo.at[i])

    def wo_rcp(i):
        col = pl.multiple_of(peer_half + ((1 - yy) if i == 0 else yy) * 1024, 128)
        return pltpu.make_async_remote_copy(
            wo_h.at[:, pl.ds(col, 1024)], wo_v.at[i, pl.ds(256, 256)],
            wo_ss, wo_rs, device_id=core_dev, device_id_type=MESH)

    barrier = pltpu.get_barrier_semaphore()
    for d in (1, 2, 3):
        pl.semaphore_signal(barrier, inc=1, device_id=seq_dev(d), device_id_type=MESH)
        pl.semaphore_signal(barrier, inc=1, device_id=z_dev(d), device_id_type=MESH)

    def load_body(c, carry):
        k_cp(c).start()
        v_cp(c).start()

        @pl.when(c == 2)
        def _():
            for i in range(2):
                wo_cp(i).start()
        return carry

    lens_cp.wait()

    sub8 = lax.broadcasted_iota(jnp.int32, (8, 128), 0)
    lane8 = lax.broadcasted_iota(jnp.int32, (8, 128), 1)

    def len_body(g, carry):
        r0 = pl.multiple_of(g * 8, 8)
        acc = jnp.zeros((8, 128), jnp.int32)
        for b in range(8):
            acc = jnp.where(sub8 == b, lens_s[r0 + b], acc)
        len_v[pl.ds(r0, 8), :] = acc
        return carry

    lax.fori_loop(0, ROWS // 8, len_body, 0)

    lane = lax.broadcasted_iota(jnp.int32, (ROWS, HD), 1)
    inv_freq = jnp.exp((lane % 64).astype(F32) * (-math.log(ROPE_THETA) / 64.0))
    angle = (len_v[...] - 1).astype(F32) * inv_freq
    cosv = jnp.cos(angle)
    sinv = jnp.where(lane < 64, -jnp.sin(angle), jnp.sin(angle))

    q_raw = jnp.zeros((ROWS, 2 * HD), F32)
    for i in range(NW):
        x_cp(i).wait()
        wq_cp(i).wait()
        if i == 1:
            lax.fori_loop(0, NC, load_body, 0)
        slot = i % 2
        wf_v[slot] = wq_v[pl.ds(i * WR, WR), :].astype(F32)
        w0 = wf_v[slot, pl.ds(0, WR // 2, 2), :].astype(BF16)
        w1 = wf_v[slot, pl.ds(1, WR // 2, 2), :].astype(BF16)
        w = jnp.concatenate([w0, w1], axis=1)
        q_raw = q_raw + jnp.dot(x_v[:, pl.ds(i * (WR // 2), WR // 2)], w, preferred_element_type=F32)
    for hh in range(2):
        qh = q_raw[:, hh * HD:(hh + 1) * HD]
        rot = pltpu.roll(qh, 64, 1)
        q_all[s, :, hh * HD:(hh + 1) * HD] = (qh * cosv + rot * sinv).astype(BF16)

    pl.semaphore_wait(barrier, 6)


    def q_cp(h, d, src):
        return pltpu.make_async_remote_copy(
            q_all.at[src, pl.ds(pl.multiple_of(h * RB, RB), RB)], q_all.at[src, pl.ds(pl.multiple_of(h * RB, RB), RB)],
            q_ss, q_rs.at[h], device_id=seq_dev(d), device_id_type=MESH)

    def send_q(h, carry):
        for d in (2, 1, 3):
            q_cp(h, d, s).start()
        return carry

    lax.fori_loop(0, QH, send_q, 0)
    for i in range(2):
        wo_rcp(i).start()

    scale = HD ** -0.5 * math.log2(math.e)
    col8 = lax.broadcasted_iota(jnp.int32, (8, 2 * T), 1)
    big = 1 << 20
    colkey = [jnp.where(col8 % 2 == n, col8 // 2, big) for n in range(2)]
    t_off = s * T
    row64 = lax.broadcasted_iota(jnp.int32, (64, HD), 0) % 8

    def o_cp(c, d):
        return pltpu.make_async_remote_copy(
            o_send.at[c, (s + d) % 4], o_recv.at[c, d - 1],
            o_ss, o_rs.at[c], device_id=seq_dev(d), device_id_type=MESH)

    def issue_scores(c):
        rows = pl.ds(c * RB, RB)
        arrived(q_all.at[pl.ds(0, 3), rows], q_rs.at[c])
        k_cp(c).wait()
        return pl.multiple_of(c * RB, RB)

    def scores(r0):
        qf = [q_all[i, pl.ds(r0, RB), :].astype(F32) for i in range(4)]
        for o in range(2):
            q64 = jnp.concatenate(
                [qf[i][8 * o:8 * o + 8, hh * HD:(hh + 1) * HD] for i in range(4) for hh in range(2)], axis=0)
            lhs = jnp.concatenate([jnp.where(row64 == b, q64, 0.0).astype(BF16) for b in range(8)], axis=1)
            kn = jnp.concatenate([k_v[r0 + 8 * o + b] for b in range(NX)], axis=1)
            res = lax.dot_general(lhs[:, :NX * HD], kn, (((1,), (1,)), ((), ())), preferred_element_type=F32)
            if NX < 8:
                kt = jnp.concatenate([k_v[r0 + 8 * o + b].T for b in range(NX, 8)], axis=0)
                res = res + jnp.dot(lhs[:, NX * HD:], kt, preferred_element_type=F32)
            s_scr[o] = res

    def softmax(c):
        r0 = pl.multiple_of(c * RB, RB)
        ml = [jnp.zeros((8, 128), F32) for _ in range(4)]
        for o in range(2):
            lim = len_v[pl.ds(r0 + 8 * o, 8), :] - t_off
            lim = jnp.concatenate([lim] * 4, axis=1)
            mask = [colkey[n] < lim for n in range(2)]
            for g2 in range(4):
                ps = []
                for g in (2 * g2, 2 * g2 + 1):
                    zz = jnp.where(mask[g // 4], s_scr[o, 8 * g:8 * g + 8, :] * scale, NEG)
                    m = jnp.maximum(jnp.max(zz, axis=1, keepdims=True), FLOOR)
                    p = jnp.exp2(zz - m)
                    l = jnp.sum(p, axis=1, keepdims=True)
                    ml[g // 2] = jnp.where(lane8 == 4 * o + g % 2, m, ml[g // 2])
                    ml[g // 2] = jnp.where(lane8 == 4 * o + 2 + g % 2, l, ml[g // 2])
                    ps.append(p)
                p_scr[o, 16 * g2:16 * g2 + 16, :] = jnp.concatenate(ps, axis=0).astype(BF16)
        for i in range(4):
            o_send[c, i, pl.ds(2 * RB, 8), :] = ml[i]

    def weighted(c):
        r0 = pl.multiple_of(c * RB, RB)
        for o in range(2):
            vc = jnp.concatenate([v_v[r0 + 8 * o + b] for b in range(8)], axis=1)
            res = jnp.dot(p_scr[o], vc, preferred_element_type=F32)
            acc = jnp.where(row64 == 0, res[:, :HD], 0.0)
            for b in range(1, 8):
                acc = jnp.where(row64 == b, res[:, b * HD:(b + 1) * HD], acc)
            for i in range(4):
                for hh in range(2):
                    g = 2 * i + hh
                    o_send[c, i, pl.ds(hh * RB + 8 * o, 8), :] = acc[8 * g:8 * g + 8]

    def send_o(c):
        for d in (2, 3, 1):
            o_cp(c, d).start()

    def attention(k):
        done = 0 if k == 0 else k - 1
        if k != 1:
            v_cp(done).wait()
        if k < NC:
            r0 = issue_scores(k)
        if k > 1:
            softmax(done)
        if k < NC:
            scores(r0)
        if k == 0:
            softmax(done)
        if k != 1:
            weighted(done)
            send_o(done)

    def a_cp(c):
        rows = pl.ds(pl.multiple_of(c * RB, RB), RB)
        return pltpu.make_async_remote_copy(
            at_own.at[rows], at_peer.at[rows], a_ss, a_rs.at[c],
            device_id=core_dev, device_id_type=MESH)

    def stage_b(c):
        arrived(o_recv.at[c], o_rs.at[c])
        mls = [o_send[c, s, pl.ds(2 * RB, 8), :]] + [o_recv[c, d, pl.ds(2 * RB, 8), :] for d in range(3)]
        mx = jnp.maximum(jnp.maximum(mls[0], mls[1]), jnp.maximum(mls[2], mls[3]))
        is_m = (lane8 % 4) < 2
        fs = [jnp.exp2(jnp.where(is_m, v - mx, 0.0)) for v in mls]
        tot = sum(f * pltpu.roll(v, 126, 1) for f, v in zip(fs, mls))
        tot = jnp.where(is_m, tot, 1.0)
        gs = [f / tot for f in fs]
        r0 = pl.multiple_of(c * RB, RB)
        for hh in range(2):
            parts = []
            for o in range(2):
                idx = 4 * o + hh
                rows = pl.ds(hh * RB + 8 * o, 8)
                acc = jnp.broadcast_to(gs[0][:, idx:idx + 1], (8, HD)) * o_send[c, s, rows, :]
                for d in range(3):
                    acc = acc + jnp.broadcast_to(gs[d + 1][:, idx:idx + 1], (8, HD)) * o_recv[c, d, rows, :]
                parts.append(acc)
            at_own[pl.ds(r0, RB), hh * HD:(hh + 1) * HD] = jnp.concatenate(parts, axis=0).astype(BF16)
        a_cp(c).start()

    def y_cp(c):
        return pltpu.make_async_remote_copy(
            y_send.at[c], y_recv.at[c], y_ss, y_rs.at[c], device_id=y_dev, device_id_type=MESH)

    def stage_c(c):
        if c == 0:
            for i in range(2):
                wo_cp(i).wait()
            arrived(wo_v.at[:, pl.ds(256, 256)], wo_rs)
        a_cp(c).wait_recv()
        r0 = pl.multiple_of(c * RB, RB)
        at = jnp.concatenate([at_own[pl.ds(r0, RB), :], at_peer[pl.ds(r0, RB), :]], axis=1)
        if c in Z_FIRST:
            for p in range(2):
                part = jnp.dot(at, wo_v[p], preferred_element_type=F32)
                for i in range(4):
                    f_buf[slot_f(c), i, p] = part[:, i * 256:(i + 1) * 256]
            for d in (2, 1, 3):
                f_cp(c, d).start()
            return
        y_send[c] = jnp.dot(at, wo_v[0], preferred_element_type=F32)
        y_cp(c).start()
        y_keep[c] = jnp.dot(at, wo_v[1], preferred_element_type=F32)

    def slot_f(c):
        return Z_FIRST.index(c)

    def f_cp(c, d):
        i = slot_f(c)
        return pltpu.make_async_remote_copy(
            f_buf.at[i, (z + d) % 4], f_recv.at[i, d - 1],
            f_ss, z_rs.at[c], device_id=z_dev(d), device_id_type=MESH)

    def g_cp(c):
        i = slot_f(c)
        return pltpu.make_async_remote_copy(
            g_buf.at[i, 0], g_recv.at[i], g_ss, y_rs.at[c], device_id=y_dev, device_id_type=MESH)

    def z_cp(c, d):
        return pltpu.make_async_remote_copy(
            z_buf.at[c, (z + d) % 4], z_recv.at[c, d - 1],
            z_ss, z_rs.at[c], device_id=z_dev(d), device_id_type=MESH)

    def stage_d(c):
        if c in Z_FIRST:
            i = slot_f(c)
            arrived(f_recv.at[i], z_rs.at[c])
            g_buf[i] = (f_buf[i, z] + f_recv[i, 0]) + (f_recv[i, 1] + f_recv[i, 2])
            g_cp(c).start()
            return
        y_cp(c).wait_recv()
        tot = y_keep[c] + y_recv[c]
        for i in range(4):
            z_buf[c, i] = tot[:, i * 256:(i + 1) * 256]
        for d in (2, 1, 3):
            z_cp(c, d).start()

    def ez_cp(c, d, src):
        rows = pl.ds(pl.multiple_of(c * RB, RB), RB)
        cols = pl.ds(pl.multiple_of(own_col + src * 256, 128), 256)
        return pltpu.make_async_remote_copy(
            out_v.at[rows, cols], out_v.at[rows, cols],
            ez_ss, ez_rs.at[c], device_id=z_dev(d), device_id_type=MESH)

    def stage_e(c):
        if c in Z_FIRST:
            arrived(g_recv.at[slot_f(c)], y_rs.at[c])
        else:
            arrived(z_recv.at[c], z_rs.at[c])
        r0 = pl.multiple_of(c * RB, RB)
        cols = pl.ds(pl.multiple_of(own_col + z * 256, 128), 256)
        if c in Z_FIRST:
            tot = g_buf[slot_f(c), 1] + g_recv[slot_f(c)]
        else:
            tot = (z_buf[c, z] + z_recv[c, 0]) + (z_recv[c, 1] + z_recv[c, 2])
        out_v[pl.ds(r0, RB), cols] = (x_v[pl.ds(r0, RB), cols].astype(F32) + tot).astype(BF16)
        for d in (2, 1, 3):
            ez_cp(c, d, z).start()

    def quarter(c, col):
        return out_v.at[pl.ds(pl.multiple_of(c * RB, RB), RB), pl.ds(pl.multiple_of(col, 128), 1024)]

    def ey_cp(c, col):
        q = quarter(c, col)
        return pltpu.make_async_remote_copy(q, q, ey_ss, ey_rs.at[c], device_id=y_dev, device_id_type=MESH)

    def ec_cp(c, col):
        q = quarter(c, col)
        return pltpu.make_async_remote_copy(q, q, ec_ss, ec_rs.at[c], device_id=core_dev, device_id_type=MESH)

    def ed_cp(c, col):
        q = quarter(c, col)
        return pltpu.make_async_remote_copy(q, q, ed_ss, ed_rs.at[c], device_id=core_dev, device_id_type=MESH)

    def stage_f(c):
        arrived(out_v.at[pl.ds(c * RB, RB), pl.ds(0, 768)], ez_rs.at[c])
        ey_cp(c, own_col).start()
        ec_cp(c, own_col).start()

    def stage_g(c):
        ey_cp(c, oth_col).wait_recv()
        ed_cp(c, oth_col).start()

    def stage_h(c):
        ec_cp(c, peer_half + yy * 1024).wait_recv()
        ed_cp(c, peer_half + (1 - yy) * 1024).wait_recv()

    stages = (attention, stage_b, stage_c, stage_d, stage_e, stage_f, stage_g, stage_h)
    for stage, c in ORDER:
        stages[stage](c)

    sent(q_all.at[pl.ds(0, 3)], q_ss)
    sent(wo_v.at[:, pl.ds(0, 256)], wo_ss)
    sent(o_recv, o_ss)
    sent(at_own, a_ss)
    sent(y_send.at[pl.ds(0, NC - NF)], y_ss)
    sent(z_recv.at[pl.ds(0, NC - NF)], z_ss)
    sent(f_recv, f_ss)
    sent(g_recv, g_ss)
    sent(out_v.at[:, pl.ds(0, 768)], ez_ss)
    for sem in (ey_ss, ec_ss, ed_ss):
        sent(out_v.at[:, pl.ds(0, 1024)], sem)


def solution(mesh):
    def local_step(x_hidden, seq_lens, k_loc, v_loc, wq_loc, wo_loc):
        k2 = k_loc.reshape(ROWS, 2 * T, HD)
        v2 = v_loc.reshape(ROWS, 2 * T, HD)
        wq2 = wq_loc.reshape(2 * D, HD)
        wo2 = wo_loc.reshape(2 * HD, D)
        dma = pltpu.SemaphoreType.DMA
        any_spec = pl.BlockSpec(memory_space=pltpu.HBM)
        return pl.pallas_call(
            kernel,
            out_shape=jax.ShapeDtypeStruct((ROWS, D), BF16),
            in_specs=[any_spec] * 6,
            out_specs=pl.BlockSpec(memory_space=pltpu.VMEM),
            scratch_shapes=[
                pltpu.SMEM((ROWS,), jnp.int32),
                pltpu.VMEM((ROWS, D), BF16),
                pltpu.VMEM((ROWS, 2 * T, HD), BF16),
                pltpu.VMEM((ROWS, 2 * T, HD), BF16),
                pltpu.VMEM((2 * D, HD), BF16),
                pltpu.VMEM((2, WR, HD), F32),
                pltpu.VMEM((2, 512, 1024), BF16),
                pltpu.VMEM((ROWS, 128), jnp.int32),
                pltpu.VMEM((4, ROWS, 2 * HD), BF16),
                pltpu.VMEM((NC, 4, OR_, HD), F32),
                pltpu.VMEM((NC, 3, OR_, HD), F32),
                pltpu.VMEM((ROWS, 2 * HD), BF16),
                pltpu.VMEM((ROWS, 2 * HD), BF16),
                pltpu.VMEM((NC, RB, 1024), F32),
                pltpu.VMEM((NC, RB, 1024), F32),
                pltpu.VMEM((NC, RB, 1024), F32),
                pltpu.VMEM((NC, 4, RB, 256), F32),
                pltpu.VMEM((NC, 3, RB, 256), F32),
                pltpu.VMEM((NF, 4, 2, RB, 256), F32),
                pltpu.VMEM((NF, 3, 2, RB, 256), F32),
                pltpu.VMEM((NF, 2, RB, 256), F32),
                pltpu.VMEM((NF, RB, 256), F32),
                pltpu.VMEM((2, 64, 2 * T), F32),
                pltpu.VMEM((2, 64, 2 * T), BF16),
                dma(()), dma((NW,)), dma((NW,)), dma((NC,)), dma((NC,)), dma((2,)),
                dma(()), dma(()),
                dma(()), dma((NC,)),
                dma(()), dma((NC,)),
                dma(()), dma((NC,)),
                dma(()), dma((NC,)),
                dma(()), dma((NC,)),
                dma(()), dma(()),
                dma(()), dma((NC,)),
                dma(()), dma((NC,)),
                dma(()), dma((NC,)),
                dma(()), dma((NC,)),
            ],
            compiler_params=pltpu.CompilerParams(
                collective_id=0, has_side_effects=True, vmem_limit_bytes=52 * 1024 * 1024),
            name="decode",
        )(seq_lens, x_hidden, k2, v2, wq2, wo2)

    return jax.shard_map(
        local_step,
        mesh=mesh,
        in_specs=(P('dp', None), P('dp'), P('dp', 'seq', 'kvh', None), P('dp', 'seq', 'kvh', None),
                  P(None, ('kvh', 'seq'), None), P(('kvh', 'seq'), None, None)),
        out_specs=P('dp', None),
        check_vma=False)
```
